128 devices in a mesh: vec: 4 (over z), row: 32 (over x, y, core).
Axes of the slice: x: 4, y: 4, z: 4, core: 2. Of those that a mesh axis runs over, the one named last changes fastest.
Arguments:
- chol_vectors: float32 [128, 1024, 1024], P('vec', 'row'), may hold values from -16 to 16, as said below
Outputs:
- rotated: float32 [128, 1024, 1024], P('vec', 'row')
- rotation: float32 [1024, 1024], P('row')
The draws below stay inside these ranges and needn't reach their ends.
Inputs may be any that keep to these rules, and one draw needn't show every extreme that they name: Every matrix chol_vectors[P] is symmetric in its last two dimensions.
All inputs are finite; a program needn't handle non-finite values.
Results may differ from the reference program's by a relative error of at most 0.00014.
Values sent between devices are 32-bit elements; how exact they have to be, the bound alone decides.
A program may use at most 128 MiB of HBM per device.

```python
import jax
import jax.numpy as jnp
from jax import lax

N = 1024
ITERS = 2
NP = 128


def draw_chol_vectors(key, part):
    first = jax.random.fold_in(jax.random.fold_in(key, 17), 0)
    values = jax.random.normal(first, (NP, N, N), jnp.float32)
    values = jnp.clip(values, -8.0, 8.0)
    return 0.5 * (values + jnp.transpose(values, (0, 2, 1)))


def setup_inputs(seed: int = 0) -> dict:
    seeds = jax.random.split(jax.random.key(seed), 2)
    chol_vectors = draw_chol_vectors(jax.random.fold_in(seeds[1], 71), 0)
    return dict(chol_vectors=chol_vectors)


def transform(matrix, step):
    left = jnp.dot(matrix, step, precision=lax.Precision.HIGHEST)
    return jnp.dot(left.T, step, precision=lax.Precision.HIGHEST)

def reference(chol_vectors):
    current = chol_vectors
    identity = jnp.eye(N, dtype=jnp.float32)
    rotation = identity
    for iteration in range(ITERS):
        diagonal = jnp.diagonal(current, axis1=1, axis2=2)
        gradient = jnp.einsum('pjk,pj->jk', current, diagonal, precision=lax.Precision.HIGHEST)
        gradient = gradient - jnp.einsum('pjk,pk->jk', current, diagonal, precision=lax.Precision.HIGHEST)
        norm = jnp.sqrt(jnp.sum(gradient * gradient) / (N * N) + 1e-06)
        generator = 0.2 / jnp.sqrt(jnp.float32(N)) * gradient / norm
        step = identity + generator + 0.5 * jnp.dot(generator, generator, precision=lax.Precision.HIGHEST)
        if iteration == 0:
            rotation = step
        else:
            rotation = jnp.dot(rotation, step, precision=lax.Precision.HIGHEST)
        current = lax.map(lambda matrix: transform(matrix, step), current)
    return (current, rotation)
```

```python
import functools

import jax
import jax.numpy as jnp
from jax import lax
from jax.experimental import pallas as pl
from jax.experimental.pallas import tpu as pltpu
from jax.sharding import PartitionSpec as P

N = 1024
NV = 4
NR = 32
VECS = 32
ROWS = 32
GROUPS = 4
GW = N // GROUPS
GP = VECS // GROUPS
STEP_GAIN = 0.2
PARTS = ((0, 384, "zyx"), (384, 384, "xzy"), (768, 256, "yxz"))
MESH = pl.DeviceIdType.MESH
F32 = jnp.float32
BF16 = jnp.bfloat16


def split(x):
    high = x.astype(BF16)
    return high, (x - high.astype(F32)).astype(BF16)


def dot3(ah, al, bh, bl):
    dot = functools.partial(jnp.dot, preferred_element_type=F32)
    return dot(ah, bh) + dot(ah, bl) + dot(al, bh)


def kernel(
    x_ref, out_ref, rot_ref,
    xf, dbuf, own, zin, full1, full2, gf, s1h, s1l, s2h, s2l, s2th, s2tl,
    l1, l1th, l1tl, dpart, din, dfull, zbuf, ah, al, stage, rh, rl,
    x_sem, zs_s, zs_r, ag_s, ag_r, co_s, co_r, d_s, d_r, db_s, db_r, big_s, big_r, out_sem,
):
    v = lax.axis_index("vec")
    r = lax.axis_index("row")
    cx, cy, cc = r // 8, (r // 2) % 4, r % 2

    load = pltpu.make_async_copy(x_ref, xf, x_sem)
    load.start()
    barrier = pltpu.get_barrier_semaphore()

    @pl.loop(1, NR)
    def _(k):
        pl.semaphore_signal(barrier, inc=1, device_id=(v, (r + k) % NR), device_id_type=MESH)

    @pl.loop(1, NV)
    def _(k):
        pl.semaphore_signal(barrier, inc=1, device_id=((v + k) % NV, r), device_id_type=MESH)

    load.wait()

    window = pl.multiple_of((r // 4) * 128, 128)
    lane = lax.broadcasted_iota(jnp.int32, (8, ROWS, 128), 2)
    sub = lax.broadcasted_iota(jnp.int32, (8, ROWS, 128), 1)

    @pl.loop(0, VECS // 8)
    def _(g):
        block = xf[pl.ds(g * 8, 8), :, pl.ds(window, 128)]
        picked = jnp.where(lane == sub + (r % 4) * ROWS, block, 0.0)
        dbuf[pl.ds(g * 8, 8)] = jnp.broadcast_to(
            jnp.sum(picked, axis=2, keepdims=True), (8, ROWS, 128)
        )

    def weighted(source, weight_of):
        for t in range(0, N, 256):
            def body(p, acc):
                return acc + source(p, t) * weight_of(p, t)
            acc = lax.fori_loop(0, VECS, body, jnp.zeros((ROWS, 256), F32), unroll=4)
            own[:, :, pl.ds(t, 256)] = acc.reshape(NV, 8, 256)

    def wide(d):
        return jnp.concatenate([d, d], axis=1)

    weighted(lambda p, t: xf[p, :, pl.ds(t, 256)], lambda p, t: wide(dbuf[p]))
    pl.semaphore_wait(barrier, NR - 1 + NV - 1)

    def exchange(full, which, filler):
        full6 = full.reshape(4, 4, 2, 4, 8, N)

        def zcopy(k):
            to = (v + k) % NV
            return pltpu.make_async_remote_copy(
                src_ref=own.at[to], dst_ref=zin.at[which, k - 1],
                send_sem=zs_s.at[which, k - 1], recv_sem=zs_r.at[which, k - 1],
                device_id=(to, r), device_id_type=MESH)

        zcopies = [zcopy(k) for k in range(1, NV)]
        for c in zcopies:
            c.start()
        for c in zcopies:
            c.wait()
        piece = own[v] + zin[which, 0] + zin[which, 1] + zin[which, 2]
        full6[cx, cy, cc, v] = piece

        def region(part, have, at):
            lo, n, _ = PARTS[part]
            ix, iy, iz = (
                pl.ds(0, 4) if d in have else pl.ds(at[d], 1) for d in "xyz")
            return full6.at[ix, iy, pl.ds(at["c"], 1), iz, :, pl.ds(lo, n)]

        me = dict(x=cx, y=cy, z=v, c=cc)

        def peer(d, k):
            at = dict(me)
            at[d] = (me[d] + k) % 4
            return at

        def device(at):
            return (at["z"], at["x"] * 8 + at["y"] * 2 + at["c"])

        def ag(part, phase, k):
            order = PARTS[part][2]
            have = order[:phase]
            return pltpu.make_async_remote_copy(
                src_ref=region(part, have, me), dst_ref=region(part, have, me),
                send_sem=ag_s.at[which, part, phase, k - 1],
                recv_sem=ag_r.at[which, part, phase, k - 1],
                device_id=device(peer(order[phase], k)), device_id_type=MESH)

        def ag_in(part, phase, k):
            order = PARTS[part][2]
            have = order[:phase]
            at = peer(order[phase], 4 - k)
            return at, pltpu.make_async_remote_copy(
                src_ref=region(part, have, at), dst_ref=region(part, have, at),
                send_sem=ag_s.at[which, part, phase, k - 1],
                recv_sem=ag_r.at[which, part, phase, k - 1],
                device_id=device(at), device_id_type=MESH)

        def core(part, phase, k, at):
            have = PARTS[part][2][:phase]
            return pltpu.make_async_remote_copy(
                src_ref=region(part, have, at), dst_ref=region(part, have, at),
                send_sem=co_s.at[which, part, phase, k],
                recv_sem=co_r.at[which, part, phase, k],
                device_id=device(dict(me, c=1 - cc)), device_id_type=MESH)

        sends = []
        for phase in range(4):
            for part in range(3):
                if phase:
                    for k in (1, 3, 2):
                        at, incoming = ag_in(part, phase - 1, k)
                        incoming.wait_recv()
                        c = core(part, phase - 1, k, at)
                        c.start()
                        sends.append((c, part, phase - 1, k, at))
                if phase < 3:
                    for k in (2, 1, 3):
                        c = ag(part, phase, k)
                        c.start()
                        sends.append((c,))
                if phase == 0:
                    c = core(part, 0, 0, me)
                    c.start()
                    sends.append((c, part, 0, 0, me))
            if phase < 3:
                filler(phase)
        for s in sends:
            if len(s) > 1:
                _, part, phase, k, at = s
                core(part, phase, k, dict(at, c=1 - cc)).wait_recv()
        for s in sends:
            s[0].wait_send()

    def nothing(phase):
        pass

    exchange(full1, 0, nothing)

    def antisymmetric(full, high, low):
        def body(i, acc):
            at = pl.multiple_of(i * 128, 128)
            strip = full[pl.ds(at, 128), :] - full[:, pl.ds(at, 128)].T
            gf[pl.ds(at, 128), :] = strip
            h, l = split(strip)
            high[pl.ds(at, 128), :] = h
            low[pl.ds(at, 128), :] = l
            square = strip * strip
            return acc + jnp.sum(square.reshape(16, 8, N), axis=0)
        acc = lax.fori_loop(0, N // 128, body, jnp.zeros((8, N), F32))
        total = jnp.sum(jnp.sum(acc, axis=1, keepdims=True), axis=0, keepdims=True)
        norm = jnp.sqrt(total / (N * N) + 1e-06)
        return (STEP_GAIN / (N ** 0.5)) / norm

    def tiles(m, n, body):
        @pl.loop(0, (N // m) * (N // n))
        def _(t):
            i = pl.multiple_of((t // (N // n)) * m, m)
            j = pl.multiple_of((t % (N // n)) * n, n)
            body(i, j)

    def eye(i, j, m, n):
        rows = lax.broadcasted_iota(jnp.int32, (m, n), 0) + i
        cols = lax.broadcasted_iota(jnp.int32, (m, n), 1) + j
        return (rows == cols).astype(F32)

    scale = antisymmetric(full1, ah, al)

    def step1(i, j):
        rows, cols = pl.ds(i, 256), pl.ds(j, 256)
        sq = dot3(ah[rows, :], al[rows, :], ah[:, cols], al[:, cols])
        s = eye(i, j, 256, 256) + scale * gf[rows, cols] + (0.5 * scale * scale) * sq
        h, l = split(s)
        s1h[rows, cols] = h
        s1l[rows, cols] = l

    tiles(256, 256, step1)

    def left(i, j):
        rows, cols = pl.ds(i, 256), pl.ds(j, 256)
        xh, xl = split(xf[pl.ds(i // ROWS, 8), :, :].reshape(256, N))
        l1[pl.ds(i // ROWS, 8), :, cols] = dot3(xh, xl, s1h[:, cols], s1l[:, cols]).reshape(8, ROWS, 256)

    tiles(256, 256, left)

    mine = pl.ds(pl.multiple_of(r * ROWS, ROWS), ROWS)
    for t in range(8):
        cols = pl.ds(t * 128, 128)
        weight = s1h[mine, cols].astype(F32) + s1l[mine, cols].astype(F32)

        @pl.loop(0, VECS, unroll=4)
        def _(p):
            dpart[p, pl.ds(t, 1), :] = jnp.sum(l1[p, :, cols] * weight, axis=0, keepdims=True)

    def dsend(k):
        to = (r + k) % NR
        return pltpu.make_async_remote_copy(
            src_ref=dpart.at[to], dst_ref=din.at[k], send_sem=d_s.at[k], recv_sem=d_r.at[k],
            device_id=(v, to), device_id_type=MESH)

    def dback(k):
        to = (r + k) % NR
        return pltpu.make_async_remote_copy(
            src_ref=din.at[0], dst_ref=dfull.at[r], send_sem=db_s.at[k], recv_sem=db_r.at[k],
            device_id=(v, to), device_id_type=MESH)

    def dback_in(k):
        source = (r + NR - k) % NR
        return pltpu.make_async_remote_copy(
            src_ref=din.at[0], dst_ref=dfull.at[source], send_sem=db_s.at[k], recv_sem=db_r.at[k],
            device_id=(v, source), device_id_type=MESH)

    @pl.loop(1, NR)
    def _(k):
        dsend(k).start()

    @pl.loop(1, NR)
    def _(k):
        dsend(k).wait_recv()

    total = dpart[r] + jnp.sum(din[pl.ds(1, NR - 1)], axis=0)
    din[0] = total
    dfull[r] = total

    @pl.loop(1, NR)
    def _(k):
        dback(k).start()

    def transposed(i):
        at = pl.multiple_of(i * 128, 128)
        strip = l1[pl.ds(i * 4, 4), :, :].reshape(128, N).T
        h, l = split(strip)
        l1th[:, pl.ds(at, 128)] = h
        l1tl[:, pl.ds(at, 128)] = l

    @pl.loop(0, N // 128)
    def _(i):
        transposed(i)

    @pl.loop(1, NR)
    def _(k):
        dback_in(k).wait_recv()

    @pl.loop(1, NR)
    def _(k):
        dsend(k).wait_send()
        dback(k).wait_send()

    for t in range(8):
        cols = pl.ds(t * 128, 128)
        def body(p, acc):
            return acc + l1[p, :, cols] * dfull[p, pl.ds(t, 1), :]
        acc = lax.fori_loop(0, VECS, body, jnp.zeros((ROWS, 128), F32), unroll=4)
        own[:, :, cols] = acc.reshape(NV, 8, 128)

    exchange(full2, 1, nothing)

    @pl.loop(0, N // 128)
    def _(i):
        at = pl.multiple_of(i * 128, 128)
        h, l = split(full2[pl.ds(at, 128), :].T)
        ah[:, pl.ds(at, 128)] = h
        al[:, pl.ds(at, 128)] = l

    def own2(i, j):
        rows, cols = pl.ds(i, 256), pl.ds(j, 256)
        gtmp[rows, cols] = dot3(ah[rows, :], al[rows, :], s1h[:, cols], s1l[:, cols])

    gtmp = stage
    tiles(256, 256, own2)
    scale2 = antisymmetric(gtmp, ah, al)

    def step2(i, j):
        rows, cols = pl.ds(i, 256), pl.ds(j, 256)
        sq = dot3(ah[rows, :], al[rows, :], ah[:, cols], al[:, cols])
        even = eye(i, j, 256, 256) + (0.5 * scale2 * scale2) * sq
        odd = scale2 * gf[rows, cols]
        h, l = split(even + odd)
        s2h[rows, cols] = h
        s2l[rows, cols] = l
        h, l = split(even - odd)
        s2th[rows, cols] = h
        s2tl[rows, cols] = l

    tiles(256, 256, step2)

    def big(g, k):
        to = (r + k) % NR
        lanes = pl.ds(g * GW, GW)
        return pltpu.make_async_remote_copy(
            src_ref=stage.at[pl.ds(pl.multiple_of(to * ROWS, ROWS), ROWS), lanes],
            dst_ref=zbuf.at[mine, lanes],
            send_sem=big_s.at[g, k], recv_sem=big_r.at[g, k],
            device_id=(v, to), device_id_type=MESH)

    def big_in(g, k):
        source = (r + NR - k) % NR
        lanes = pl.ds(g * GW, GW)
        return pltpu.make_async_remote_copy(
            src_ref=stage.at[mine, lanes],
            dst_ref=zbuf.at[pl.ds(pl.multiple_of(source * ROWS, ROWS), ROWS), lanes],
            send_sem=big_s.at[g, k], recv_sem=big_r.at[g, k],
            device_id=(v, source), device_id_type=MESH)

    for g in range(GROUPS):
        lanes = pl.ds(g * GW, GW)

        @pl.loop(0, 4)
        def _(i):
            rows = pl.ds(pl.multiple_of(i * 256, 256), 256)
            stage[rows, lanes] = dot3(s2th[rows, :], s2tl[rows, :], l1th[:, lanes], l1tl[:, lanes])

        zbuf[mine, lanes] = stage[mine, lanes]

        @pl.loop(1, NR)
        def _(k):
            big(g, k).start()

    def rotation(i, j):
        rows, cols = pl.ds(i, 256), pl.ds(j, 256)
        h, l = split(dot3(s1h[rows, :], s1l[rows, :], s2h[:, cols], s2l[:, cols]))
        rh[rows, cols] = h
        rl[rows, cols] = l

    tiles(256, 256, rotation)
    rot_ref[...] = rh[mine, :].astype(F32) + rl[mine, :].astype(F32)

    group = lax.broadcasted_iota(jnp.int32, (ROWS, 128), 1) // ROWS

    def put(g):
        return pltpu.make_async_copy(xf.at[pl.ds(g * GP, GP)], out_ref.at[pl.ds(g * GP, GP)], out_sem.at[g])

    for g in range(GROUPS):
        @pl.loop(1, NR)
        def _(k):
            big_in(g, k).wait_recv()

        @pl.loop(0, 8)
        def _(b4):
            for q in range(GW // 128):
                blocks = [
                    zbuf[pl.ds(pl.multiple_of(b4 * 128 + b * ROWS, ROWS), ROWS), pl.ds(g * GW + q * 128, 128)]
                    for b in range(4)]
                for p in range(4):
                    out = blocks[p]
                    for b in range(4):
                        if b != p:
                            turned = pltpu.roll(blocks[b], (ROWS * (b - p)) % 128, 1)
                            out = jnp.where(group == b, turned, out)
                    h, l = split(out)
                    rows = pl.ds((q * 4 + p) * ROWS, ROWS)
                    cols = pl.ds(pl.multiple_of(b4 * 128, 128), 128)
                    ah[rows, cols] = h
                    al[rows, cols] = l

        @pl.loop(0, 4)
        def _(j):
            cols = pl.ds(pl.multiple_of(j * 256, 256), 256)
            res = dot3(ah[pl.ds(0, GW), :], al[pl.ds(0, GW), :], rh[:, cols], rl[:, cols])
            xf[pl.ds(g * GP, GP), :, cols] = res.reshape(GP, ROWS, 256)

        put(g).start()

    for g in range(GROUPS):
        put(g).wait()

        @pl.loop(1, NR)
        def _(k):
            big(g, k).wait_send()


def shards(chol_vectors):
    full = pltpu.VMEM((N, N), F32)
    half = pltpu.VMEM((N, N), BF16)
    sem = pltpu.SemaphoreType.DMA
    return pl.pallas_call(
        kernel,
        out_shape=(
            jax.ShapeDtypeStruct((VECS, ROWS, N), F32),
            jax.ShapeDtypeStruct((ROWS, N), F32),
        ),
        in_specs=[pl.BlockSpec(memory_space=pl.ANY)],
        out_specs=(pl.BlockSpec(memory_space=pl.ANY), pl.BlockSpec(memory_space=pltpu.VMEM)),
        scratch_shapes=[
            pltpu.VMEM((VECS, ROWS, N), F32),
            pltpu.VMEM((VECS, ROWS, 128), F32),
            pltpu.VMEM((NV, 8, N), F32),
            pltpu.VMEM((2, NV - 1, 8, N), F32),
            full,
            full,
            full,
            half, half, half, half, half, half,
            pltpu.VMEM((VECS, ROWS, N), F32),
            half, half,
            pltpu.VMEM((VECS, 8, 128), F32),
            pltpu.VMEM((NR, 8, 128), F32),
            pltpu.VMEM((NR, 8, 128), F32),
            full,
            half, half,
            full,
            half, half,
            sem,
            sem((2, 3)), sem((2, 3)),
            sem((2, 3, 3, 3)), sem((2, 3, 3, 3)),
            sem((2, 3, 3, 4)), sem((2, 3, 3, 4)),
            sem((NR,)), sem((NR,)), sem((NR,)), sem((NR,)),
            sem((GROUPS, NR)), sem((GROUPS, NR)),
            sem((GROUPS,)),
        ],
        compiler_params=pltpu.CompilerParams(
            collective_id=0, has_side_effects=True, vmem_limit_bytes=67043328
        ),
    )(chol_vectors)


def solution(mesh):
    return jax.shard_map(
        shards,
        mesh=mesh,
        in_specs=(P("vec", "row", None),),
        out_specs=(P("vec", "row", None), P("row", None)),
        check_vma=False,
    )
```

```python
import functools

import jax
import jax.numpy as jnp
from jax import lax
from jax.experimental import pallas as pl
from jax.experimental.pallas import tpu as pltpu
from jax.sharding import PartitionSpec as P

N = 1024
NV = 4
NR = 32
VECS = 32
ROWS = 32
GROUPS = 4
GW = N // GROUPS
GP = VECS // GROUPS
STEP_GAIN = 0.2
VMEM_LIMIT = 58 << 20
PARTS = ((0, 384, "zyx"), (384, 384, "xzy"), (768, 256, "yxz"))
OFFSETS = tuple(sorted(
    ((dx, dy, dc) for dx in range(4) for dy in range(4) for dc in range(2) if dx or dy or dc),
    key=lambda o: -(min(o[0], 4 - o[0]) + min(o[1], 4 - o[1]))))
MESH = pl.DeviceIdType.MESH
F32 = jnp.float32
BF16 = jnp.bfloat16


def split(x):
    high = x.astype(BF16)
    return high, (x - high.astype(F32)).astype(BF16)


def dot3(ah, al, bh, bl):
    dot = functools.partial(jnp.dot, preferred_element_type=F32)
    return dot(ah, bh) + dot(ah, bl) + dot(al, bh)


def kernel(
    x_ref, out_ref, rot_ref,
    xf, dbuf, own, zin, full1, full2, gf, s1h, s1l, s2h, s2l,
    l1, l1th, l1tl, dpart, din, dfull, zbuf, ah, al, stage, rh, rl, wh, wl, lh, ll,
    x_sem, zs_s, zs_r, ag_s, ag_r, co_s, co_r, d_sem, big_s, big_r,
):
    v = lax.axis_index("vec")
    r = lax.axis_index("row")
    cx, cy, cc = r // 8, (r // 2) % 4, r % 2

    load = pltpu.make_async_copy(x_ref, xf, x_sem)
    load.start()
    barrier = pltpu.get_barrier_semaphore()

    @pl.loop(1, NR)
    def _(k):
        pl.semaphore_signal(barrier, inc=1, device_id=(v, (r + k) % NR), device_id_type=MESH)

    @pl.loop(1, NV)
    def _(k):
        pl.semaphore_signal(barrier, inc=1, device_id=((v + k) % NV, r), device_id_type=MESH)

    load.wait()

    window = pl.multiple_of((r // 4) * 128, 128)
    lane = lax.broadcasted_iota(jnp.int32, (8, ROWS, 128), 2)
    sub = lax.broadcasted_iota(jnp.int32, (8, ROWS, 128), 1)

    @pl.loop(0, VECS // 8)
    def _(g):
        block = xf[pl.ds(g * 8, 8), :, pl.ds(window, 128)]
        picked = jnp.where(lane == sub + (r % 4) * ROWS, block, 0.0)
        dbuf[pl.ds(g * 8, 8)] = jnp.broadcast_to(
            jnp.sum(picked, axis=2, keepdims=True), (8, ROWS, 128)
        )

    def weighted(source, weight_of):
        for t in range(0, N, 256):
            def body(p, acc):
                return acc + source(p, t) * weight_of(p, t)
            acc = lax.fori_loop(0, VECS, body, jnp.zeros((ROWS, 256), F32), unroll=4)
            own[:, :, pl.ds(t, 256)] = acc.reshape(NV, 8, 256)

    def wide(d):
        return jnp.concatenate([d, d], axis=1)

    weighted(lambda p, t: xf[p, :, pl.ds(t, 256)], lambda p, t: wide(dbuf[p]))
    pl.semaphore_wait(barrier, NR - 1 + NV - 1)

    def exchange(full, which, filler):
        full6 = full.reshape(4, 4, 2, 4, 8, N)

        def zcopy(k):
            to = (v + k) % NV
            return pltpu.make_async_remote_copy(
                src_ref=own.at[to], dst_ref=zin.at[which, k - 1],
                send_sem=zs_s.at[which], recv_sem=zs_r.at[which],
                device_id=(to, r), device_id_type=MESH)

        zcopies = [zcopy(k) for k in range(1, NV)]
        for c in zcopies:
            c.start()
        def taken(ref, sem):
            pltpu.make_async_copy(ref, ref, sem).wait()

        taken(zin.at[which], zs_r.at[which])
        piece = own[v] + zin[which, 0] + zin[which, 1] + zin[which, 2]
        full6[cx, cy, cc, v] = piece

        def region(part, have, at):
            lo, n, _ = PARTS[part]
            ix, iy, iz = (
                pl.ds(0, 4) if d in have else pl.ds(at[d], 1) for d in "xyz")
            return full6.at[ix, iy, pl.ds(at["c"], 1), iz, :, pl.ds(lo, n)]

        me = dict(x=cx, y=cy, z=v, c=cc)

        def peer(d, k):
            at = dict(me)
            at[d] = (me[d] + k) % 4
            return at

        def device(at):
            return (at["z"], at["x"] * 8 + at["y"] * 2 + at["c"])

        def ag(part, phase, k):
            order = PARTS[part][2]
            have = order[:phase]
            return pltpu.make_async_remote_copy(
                src_ref=region(part, have, me), dst_ref=region(part, have, me),
                send_sem=ag_s.at[which], recv_sem=ag_r.at[which, part, phase],
                device_id=device(peer(order[phase], k)), device_id_type=MESH)

        def core(part, have, at):
            return pltpu.make_async_remote_copy(
                src_ref=region(part, have, at), dst_ref=region(part, have, at),
                send_sem=co_s.at[which], recv_sem=co_r.at[which],
                device_id=device(dict(me, c=1 - cc)), device_id_type=MESH)

        def ag_taken(part, phase):
            lo, n, _ = PARTS[part]
            taken(full.at[pl.ds(0, 24 * 4 ** phase), pl.ds(lo, n)], ag_r.at[which, part, phase])

        for phase in range(4):
            for part in range(3):
                order = PARTS[part][2]
                if phase:
                    ag_taken(part, phase - 1)
                    for k in (1, 3, 2):
                        core(part, order[:phase - 1], peer(order[phase - 1], k)).start()
                if phase < 3:
                    for k in (2, 1, 3):
                        ag(part, phase, k).start()
                if phase == 0:
                    core(part, "", me).start()
            if phase < 3:
                filler(phase)
        half_rows = full.at[pl.ds(0, N // 2), :]
        taken(half_rows, co_r.at[which])
        taken(half_rows, co_s.at[which])
        taken(zin.at[which], zs_s.at[which])
        taken(full.at[pl.ds(0, N // 2 - 8), :], ag_s.at[which])

    def nothing(phase):
        pass

    xh, xl = l1th, l1tl

    def prepare(phase):
        if phase == 0:
            @pl.loop(0, VECS // 4)
            def _(i):
                h, l = split(xf[pl.ds(i * 4, 4)].reshape(128, N))
                rows = pl.ds(pl.multiple_of(i * 128, 128), 128)
                xh[rows, :] = h
                xl[rows, :] = l

    with jax.named_scope("ex1"):
        exchange(full1, 0, prepare)

    def antisymmetric(full, high, low):
        def body(i, acc):
            at = pl.multiple_of(i * 128, 128)
            strip = full[pl.ds(at, 128), :] - full[:, pl.ds(at, 128)].T
            gf[pl.ds(at, 128), :] = strip
            h, l = split(strip)
            high[pl.ds(at, 128), :] = h
            low[pl.ds(at, 128), :] = l
            square = strip * strip
            return acc + jnp.sum(square.reshape(16, 8, N), axis=0)
        acc = lax.fori_loop(0, N // 128, body, jnp.zeros((8, N), F32))
        total = jnp.sum(jnp.sum(acc, axis=1, keepdims=True), axis=0, keepdims=True)
        norm = jnp.sqrt(total / (N * N) + 1e-06)
        return (STEP_GAIN / (N ** 0.5)) / norm

    def eye(i, j, m, n):
        rows = lax.broadcasted_iota(jnp.int32, (m, n), 0) + i
        cols = lax.broadcasted_iota(jnp.int32, (m, n), 1) + j
        return (rows == cols).astype(F32)

    with jax.named_scope("gen1"):
        scale = antisymmetric(full1, ah, al)

    def panels(body):
        @pl.loop(0, N // 256)
        def _(t):
            body(pl.ds(pl.multiple_of(t * 256, 256), 256), t * 256)

    def series(c, high, low):
        def store(rows, cols, i, j, sq):
            value = c * gf[rows, cols] + (0.5 * c * c) * sq
            h, l = split(value + eye(i, j, sq.shape[0], 256) if i <= j else value)
            high[rows, cols] = h
            low[rows, cols] = l

        for t in range(4):
            m, cols = 256 * (t + 1), pl.ds(256 * t, 256)
            sq = dot3(ah[pl.ds(0, m), :], al[pl.ds(0, m), :], ah[:, cols], al[:, cols])
            store(pl.ds(0, m), cols, 0, 256 * t, sq)
            for u in range(t):
                store(cols, pl.ds(256 * u, 256), 256 * t, 256 * u, sq[256 * u:256 * (u + 1), :].T)

    with jax.named_scope("step1"):
        series(scale, s1h, s1l)

    def left(cols, j):
        l1[:, :, cols] = dot3(xh[...], xl[...], s1h[:, cols], s1l[:, cols]).reshape(VECS, ROWS, 256)

    with jax.named_scope("left"):
        panels(left)

    mine = pl.ds(pl.multiple_of(r * ROWS, ROWS), ROWS)
    for t in range(8):
        cols = pl.ds(t * 128, 128)
        weight = s1h[mine, cols].astype(F32) + s1l[mine, cols].astype(F32)

        @pl.loop(0, VECS, unroll=8)
        def _(p):
            dpart[p, pl.ds(t, 1), :] = jnp.sum(l1[p, :, cols] * weight, axis=0, keepdims=True)

    def dsend(k):
        to = (r + k) % NR
        return pltpu.make_async_remote_copy(
            src_ref=dpart.at[to], dst_ref=din.at[k], send_sem=d_sem.at[0], recv_sem=d_sem.at[1],
            device_id=(v, to), device_id_type=MESH)

    def dback(k):
        to = (r + k) % NR
        return pltpu.make_async_remote_copy(
            src_ref=din.at[0], dst_ref=dfull.at[r], send_sem=d_sem.at[2], recv_sem=d_sem.at[3],
            device_id=(v, to), device_id_type=MESH)

    def others(sem):
        pltpu.make_async_copy(din.at[pl.ds(1, NR - 1)], din.at[pl.ds(1, NR - 1)], d_sem.at[sem]).wait()

    @pl.loop(1, NR)
    def _(k):
        dsend(k).start()

    with jax.named_scope("drecv"):
        others(1)

    total = dpart[r] + jnp.sum(din[pl.ds(1, NR - 1)], axis=0)
    din[0] = total
    dfull[r] = total

    @pl.loop(1, NR)
    def _(k):
        dback(k).start()

    def transposed(i):
        at = pl.multiple_of(i * 128, 128)
        strip = l1[pl.ds(i * 4, 4), :, :].reshape(128, N).T
        h, l = split(strip)
        l1th[:, pl.ds(at, 128)] = h
        l1tl[:, pl.ds(at, 128)] = l

    @pl.loop(0, N // 128)
    def _(i):
        transposed(i)

    with jax.named_scope("dback"):
        others(3)
    others(0)
    others(2)

    for t in range(8):
        cols = pl.ds(t * 128, 128)
        def body(p, acc):
            return acc + l1[p, :, cols] * dfull[p, pl.ds(t, 1), :]
        acc = lax.fori_loop(0, VECS, body, jnp.zeros((ROWS, 128), F32), unroll=4)
        own[:, :, cols] = acc.reshape(NV, 8, 128)

    with jax.named_scope("ex2"):
        exchange(full2, 1, nothing)

    @pl.loop(0, N // 128)
    def _(i):
        at = pl.multiple_of(i * 128, 128)
        h, l = split(full2[pl.ds(at, 128), :].T)
        ah[:, pl.ds(at, 128)] = h
        al[:, pl.ds(at, 128)] = l

    def own2(cols, j):
        stage[:, cols] = dot3(ah[...], al[...], s1h[:, cols], s1l[:, cols])

    with jax.named_scope("own2"):
        panels(own2)
    with jax.named_scope("gen2"):
        scale2 = antisymmetric(stage, ah, al)

    def partner(i, way):
        dx, dy, dc = OFFSETS[i]
        return ((cx + way * dx + 4) % 4) * 8 + ((cy + way * dy + 4) % 4) * 2 + (cc + dc) % 2

    def rows_of(device):
        return pl.ds(pl.multiple_of(device * ROWS, ROWS), ROWS)

    def big(g, i):
        to = partner(i, 1)
        lanes = pl.ds(pl.multiple_of(g * GW, GW), GW)
        return pltpu.make_async_remote_copy(
            src_ref=stage.at[rows_of(to), lanes], dst_ref=zbuf.at[mine, lanes],
            send_sem=big_s, recv_sem=big_r.at[g, OFFSETS[i][0]],
            device_id=(v, to), device_id_type=MESH)

    def big_taken(g, dx):
        ref = zbuf.at[pl.ds(0, (8 if dx else 7) * ROWS), pl.ds(g * GW, GW)]
        pltpu.make_async_copy(ref, ref, big_r.at[g, dx]).wait()

    @pl.loop(0, GROUPS)
    def _(g):
        lanes = pl.ds(pl.multiple_of(g * GW, GW), GW)
        with jax.named_scope("l2"):
            h, l = split(scale2 * dot3(ah[...], al[...], l1th[:, lanes], l1tl[:, lanes]))
            wh[...] = h
            wl[...] = l
            second = (0.5 * scale2) * dot3(ah[...], al[...], wh[...], wl[...])
            first = wh[...].astype(F32) + wl[...].astype(F32)
            stage[:, lanes] = (l1th[:, lanes].astype(F32) + l1tl[:, lanes].astype(F32)) + (second - first)
        for i in range(NR - 1):
            big(g, i).start()
        zbuf[mine, lanes] = stage[mine, lanes]

    def rotation(cols, j):
        h, l = split(dot3(s1h[...], s1l[...], s2h[:, cols], s2l[:, cols]))
        rh[:, cols] = h
        rl[:, cols] = l

    with jax.named_scope("step2"):
        series(scale2, s2h, s2l)
    with jax.named_scope("rot"):
        panels(rotation)
    rot_ref[...] = rh[mine, :].astype(F32) + rl[mine, :].astype(F32)

    group = lax.broadcasted_iota(jnp.int32, (ROWS, 128), 1) // ROWS

    def gathered(at, q, row, col):
        blocks = [
            zbuf[pl.ds(pl.multiple_of(at + b * ROWS, ROWS), ROWS), pl.ds(pl.multiple_of(q * 128, 128), 128)]
            for b in range(4)]
        for p in range(4):
            out = blocks[p]
            for b in range(4):
                if b != p:
                    turned = pltpu.roll(blocks[b], (ROWS * (b - p)) % 128, 1)
                    out = jnp.where(group == b, turned, out)
            h, l = split(out)
            rows = pl.ds(row + p * ROWS, ROWS)
            lh[rows, col] = h
            ll[rows, col] = l

    def finish(first, chunks):
        m = chunks * GW
        with jax.named_scope(f"bigwait{first}"):
            for g in range(first, first + chunks):
                for dx in range(4):
                    big_taken(g, dx)

        with jax.named_scope(f"turn{first}"):
            @pl.loop(0, 8)
            def _(b4):
                at = pl.multiple_of(b4 * 128, 128)
                for q in range(m // 128):
                    gathered(at, first * GW // 128 + q, q * 128, pl.ds(at, 128))

        with jax.named_scope(f"final{first}"):
            @pl.loop(0, 2)
            def _(j):
                cols = pl.ds(pl.multiple_of(j * 512, 512), 512)
                res = dot3(lh[pl.ds(0, m), :], ll[pl.ds(0, m), :], rh[:, cols], rl[:, cols])
                out_ref[pl.ds(first * GP, chunks * GP), :, cols] = res.reshape(chunks * GP, ROWS, 512)

    finish(0, 2)
    finish(2, 1)

    last = GROUPS - 1
    for dx in (2, 1, 3, 0):
        with jax.named_scope(f"bigwait3_{dx}"):
            big_taken(last, dx)
        at = pl.multiple_of(((cx + 4 - dx) % 4) * 256, 256)
        for b4 in range(2):
            for q in range(GW // 128):
                gathered(at + b4 * 128, last * GW // 128 + q, q * 128, pl.ds(b4 * 128, 128))

        @pl.loop(0, 2)
        def _(j):
            cols = pl.ds(pl.multiple_of(j * 512, 512), 512)
            depth, first = pl.ds(at, 256), pl.ds(0, GW)
            res = dot3(lh[first, pl.ds(0, 256)], ll[first, pl.ds(0, 256)], rh[depth, cols], rl[depth, cols])
            res = res.reshape(GP, ROWS, 512)
            if dx == 2:
                out_ref[pl.ds(last * GP, GP), :, cols] = res
            else:
                out_ref[pl.ds(last * GP, GP), :, cols] += res

    sent = stage.at[pl.ds(0, N - ROWS), :]
    pltpu.make_async_copy(sent, sent, big_s).wait()


def shards(chol_vectors):
    full = pltpu.VMEM((N, N), F32)
    half = pltpu.VMEM((N, N), BF16)
    sem = pltpu.SemaphoreType.DMA
    return pl.pallas_call(
        kernel,
        out_shape=(
            pltpu.VMEM((VECS, ROWS, N), F32),
            jax.ShapeDtypeStruct((ROWS, N), F32),
        ),
        in_specs=[pl.BlockSpec(memory_space=pl.ANY)],
        out_specs=(pl.BlockSpec(memory_space=pltpu.VMEM), pl.BlockSpec(memory_space=pltpu.VMEM)),
        scratch_shapes=[
            pltpu.VMEM((VECS, ROWS, N), F32),
            pltpu.VMEM((VECS, ROWS, 128), F32),
            pltpu.VMEM((NV, 8, N), F32),
            pltpu.VMEM((2, NV - 1, 8, N), F32),
            full,
            full,
            full,
            half, half, half, half,
            pltpu.VMEM((VECS, ROWS, N), F32),
            half, half,
            pltpu.VMEM((VECS, 8, 128), F32),
            pltpu.VMEM((NR, 8, 128), F32),
            pltpu.VMEM((NR, 8, 128), F32),
            full,
            half, half,
            full,
            half, half,
            pltpu.VMEM((N, GW), BF16), pltpu.VMEM((N, GW), BF16),
            pltpu.VMEM((2 * GW, N), BF16), pltpu.VMEM((2 * GW, N), BF16),
            sem,
            sem((2,)), sem((2,)),
            sem((2,)), sem((2, 3, 3)),
            sem((2,)), sem((2,)),
            sem((4,)),
            sem, sem((GROUPS, 4)),
        ],
        compiler_params=pltpu.CompilerParams(
            collective_id=0, has_side_effects=True, vmem_limit_bytes=VMEM_LIMIT
        ),
    )(chol_vectors)


def solution(mesh):
    return jax.shard_map(
        shards,
        mesh=mesh,
        in_specs=(P("vec", "row", None),),
        out_specs=(P("vec", "row", None), P("row", None)),
        check_vma=False,
    )
```

```python
import functools

import jax
import jax.numpy as jnp
from jax import lax
from jax.experimental import pallas as pl
from jax.experimental.pallas import tpu as pltpu
from jax.sharding import PartitionSpec as P

N = 1024
NV = 4
NR = 32
VECS = 32
ROWS = 32
GROUPS = 4
GW = N // GROUPS
GP = VECS // GROUPS
STEP_GAIN = 0.2
VMEM_LIMIT = 58 << 20
PARTS = ((0, 384, "zyx"), (384, 384, "xzy"), (768, 256, "yxz"))
OFFSETS = tuple(sorted(
    ((dx, dy, dc) for dx in range(4) for dy in range(4) for dc in range(2) if dx or dy or dc),
    key=lambda o: -(min(o[0], 4 - o[0]) + min(o[1], 4 - o[1]))))
MESH = pl.DeviceIdType.MESH
F32 = jnp.float32
BF16 = jnp.bfloat16


def split(x):
    high = x.astype(BF16)
    return high, (x - high.astype(F32)).astype(BF16)


def dot3(ah, al, bh, bl):
    dot = functools.partial(jnp.dot, preferred_element_type=F32)
    return dot(ah, bh) + dot(ah, bl) + dot(al, bh)


def kernel(
    x_ref, out_ref, rot_ref,
    xf, dbuf, own, zin, full1, full2, gf, s1h, s1l, s2h, s2l,
    l1, l1th, l1tl, dpart, din, dfull, zbuf, ah, al, stage, rh, rl, wh, wl, lh, ll, mh, ml,
    x_sem, zs_s, zs_r, ag_s, ag_r, co_s, co_r, d_sem, big_s, big_r,
):
    v = lax.axis_index("vec")
    r = lax.axis_index("row")
    cx, cy, cc = r // 8, (r // 2) % 4, r % 2

    load = pltpu.make_async_copy(x_ref, xf, x_sem)
    load.start()
    barrier = pltpu.get_barrier_semaphore()

    @pl.loop(1, NR)
    def _(k):
        pl.semaphore_signal(barrier, inc=1, device_id=(v, (r + k) % NR), device_id_type=MESH)

    @pl.loop(1, NV)
    def _(k):
        pl.semaphore_signal(barrier, inc=1, device_id=((v + k) % NV, r), device_id_type=MESH)

    load.wait()

    window = pl.multiple_of((r // 4) * 128, 128)
    lane = lax.broadcasted_iota(jnp.int32, (8, ROWS, 128), 2)
    sub = lax.broadcasted_iota(jnp.int32, (8, ROWS, 128), 1)

    @pl.loop(0, VECS // 8)
    def _(g):
        block = xf[pl.ds(g * 8, 8), :, pl.ds(window, 128)]
        picked = jnp.where(lane == sub + (r % 4) * ROWS, block, 0.0)
        dbuf[pl.ds(g * 8, 8)] = jnp.broadcast_to(
            jnp.sum(picked, axis=2, keepdims=True), (8, ROWS, 128)
        )

    def weighted(source, weight_of):
        for t in range(0, N, 256):
            def body(p, acc):
                return acc + source(p, t) * weight_of(p, t)
            acc = lax.fori_loop(0, VECS, body, jnp.zeros((ROWS, 256), F32), unroll=4)
            own[:, :, pl.ds(t, 256)] = acc.reshape(NV, 8, 256)

    def wide(d):
        return jnp.concatenate([d, d], axis=1)

    weighted(lambda p, t: xf[p, :, pl.ds(t, 256)], lambda p, t: wide(dbuf[p]))
    pl.semaphore_wait(barrier, NR - 1 + NV - 1)

    def exchange(full, which, filler, consume=None):
        full6 = full.reshape(4, 4, 2, 4, 8, N)

        def zcopy(k):
            to = (v + k) % NV
            return pltpu.make_async_remote_copy(
                src_ref=own.at[to], dst_ref=zin.at[which, k - 1],
                send_sem=zs_s.at[which], recv_sem=zs_r.at[which],
                device_id=(to, r), device_id_type=MESH)

        zcopies = [zcopy(k) for k in range(1, NV)]
        for c in zcopies:
            c.start()
        def taken(ref, sem):
            pltpu.make_async_copy(ref, ref, sem).wait()

        taken(zin.at[which], zs_r.at[which])
        piece = own[v] + zin[which, 0] + zin[which, 1] + zin[which, 2]
        full6[cx, cy, cc, v] = piece

        def region(part, have, at):
            lo, n, _ = PARTS[part]
            ix, iy, iz = (
                pl.ds(0, 4) if d in have else pl.ds(at[d], 1) for d in "xyz")
            return full6.at[ix, iy, pl.ds(at["c"], 1), iz, :, pl.ds(lo, n)]

        me = dict(x=cx, y=cy, z=v, c=cc)

        def peer(d, k):
            at = dict(me)
            at[d] = (me[d] + k) % 4
            return at

        def device(at):
            return (at["z"], at["x"] * 8 + at["y"] * 2 + at["c"])

        def ag(part, phase, k):
            order = PARTS[part][2]
            have = order[:phase]
            return pltpu.make_async_remote_copy(
                src_ref=region(part, have, me), dst_ref=region(part, have, me),
                send_sem=ag_s.at[which], recv_sem=ag_r.at[which, part, phase + (k - 1 if phase == 2 else 0)],
                device_id=device(peer(order[phase], k)), device_id_type=MESH)

        def core(part, have, at, group):
            return pltpu.make_async_remote_copy(
                src_ref=region(part, have, at), dst_ref=region(part, have, at),
                send_sem=co_s.at[which], recv_sem=co_r.at[which, part, group],
                device_id=device(dict(me, c=1 - cc)), device_id_type=MESH)

        def lanes_taken(part, rows, sem):
            lo, n, _ = PARTS[part]
            taken(full.at[pl.ds(0, rows), pl.ds(lo, n)], sem)

        for phase in range(3):
            for part in range(3):
                order = PARTS[part][2]
                if phase:
                    lanes_taken(part, 24 * 4 ** (phase - 1), ag_r.at[which, part, phase - 1])
                    for k in (1, 3, 2):
                        core(part, order[:phase - 1], peer(order[phase - 1], k), 0).start()
                for k in ((1, 3, 2) if phase == 2 else (2, 1, 3)):
                    ag(part, phase, k).start()
                if phase == 0:
                    core(part, "", me, 0).start()
            filler(phase)

        def arrived(k):
            for part in range(3):
                order = PARTS[part][2]
                lanes_taken(part, 128, ag_r.at[which, part, 2 + k - 1])
                core(part, order[:2], peer(order[2], 4 - k), k).start()

        def use(k):
            for part in range(3):
                lanes_taken(part, 128, co_r.at[which, part, k])
                if consume is not None:
                    consume(part, peer(PARTS[part][2][2], (4 - k) % 4)[PARTS[part][2][2]], k == 0)

        with jax.named_scope(f"use{which}_0"):
            use(0)
        with jax.named_scope(f"arr{which}_13"):
            arrived(1)
            arrived(3)
        with jax.named_scope(f"use{which}_1"):
            use(1)
        with jax.named_scope(f"arr{which}_2"):
            arrived(2)
        with jax.named_scope(f"use{which}_3"):
            use(3)
        with jax.named_scope(f"use{which}_2"):
            use(2)
        taken(full.at[pl.ds(0, N // 2), :], co_s.at[which])
        taken(zin.at[which], zs_s.at[which])
        taken(full.at[pl.ds(0, N // 2 - 8), :], ag_s.at[which])

    def nothing(phase):
        pass

    xh, xl = l1th, l1tl

    def prepare(phase):
        if phase == 0:
            @pl.loop(0, VECS // 4)
            def _(i):
                h, l = split(xf[pl.ds(i * 4, 4)].reshape(128, N))
                rows = pl.ds(pl.multiple_of(i * 128, 128), 128)
                xh[rows, :] = h
                xl[rows, :] = l

    with jax.named_scope("ex1"):
        exchange(full1, 0, prepare)

    def antisymmetric(full, high, low):
        def body(i, acc):
            at = pl.multiple_of(i * 128, 128)
            strip = full[pl.ds(at, 128), :] - full[:, pl.ds(at, 128)].T
            gf[pl.ds(at, 128), :] = strip
            h, l = split(strip)
            high[pl.ds(at, 128), :] = h
            low[pl.ds(at, 128), :] = l
            square = strip * strip
            return acc + jnp.sum(square.reshape(16, 8, N), axis=0)
        acc = lax.fori_loop(0, N // 128, body, jnp.zeros((8, N), F32))
        total = jnp.sum(jnp.sum(acc, axis=1, keepdims=True), axis=0, keepdims=True)
        norm = jnp.sqrt(total / (N * N) + 1e-06)
        return (STEP_GAIN / (N ** 0.5)) / norm

    def eye(i, j, m, n):
        rows = lax.broadcasted_iota(jnp.int32, (m, n), 0) + i
        cols = lax.broadcasted_iota(jnp.int32, (m, n), 1) + j
        return (rows == cols).astype(F32)

    with jax.named_scope("gen1"):
        scale = antisymmetric(full1, ah, al)

    def panels(body):
        @pl.loop(0, N // 256)
        def _(t):
            body(pl.ds(pl.multiple_of(t * 256, 256), 256), t * 256)

    def series(c, high, low):
        def store(rows, cols, i, j, sq):
            value = c * gf[rows, cols] + (0.5 * c * c) * sq
            h, l = split(value + eye(i, j, sq.shape[0], 256) if i <= j else value)
            high[rows, cols] = h
            low[rows, cols] = l

        for t in range(4):
            m, cols = 256 * (t + 1), pl.ds(256 * t, 256)
            sq = dot3(ah[pl.ds(0, m), :], al[pl.ds(0, m), :], ah[:, cols], al[:, cols])
            store(pl.ds(0, m), cols, 0, 256 * t, sq)
            for u in range(t):
                store(cols, pl.ds(256 * u, 256), 256 * t, 256 * u, sq[256 * u:256 * (u + 1), :].T)

    with jax.named_scope("step1"):
        series(scale, s1h, s1l)

    def left(cols, j):
        l1[:, :, cols] = dot3(xh[...], xl[...], s1h[:, cols], s1l[:, cols]).reshape(VECS, ROWS, 256)

    with jax.named_scope("left"):
        panels(left)

    mine = pl.ds(pl.multiple_of(r * ROWS, ROWS), ROWS)
    for t in range(8):
        cols = pl.ds(t * 128, 128)
        weight = s1h[mine, cols].astype(F32) + s1l[mine, cols].astype(F32)

        @pl.loop(0, VECS, unroll=8)
        def _(p):
            dpart[p, pl.ds(t, 1), :] = jnp.sum(l1[p, :, cols] * weight, axis=0, keepdims=True)

    def dsend(k):
        to = (r + k) % NR
        return pltpu.make_async_remote_copy(
            src_ref=dpart.at[to], dst_ref=din.at[k], send_sem=d_sem.at[0], recv_sem=d_sem.at[1],
            device_id=(v, to), device_id_type=MESH)

    def dback(k):
        to = (r + k) % NR
        return pltpu.make_async_remote_copy(
            src_ref=din.at[0], dst_ref=dfull.at[r], send_sem=d_sem.at[2], recv_sem=d_sem.at[3],
            device_id=(v, to), device_id_type=MESH)

    def others(sem):
        pltpu.make_async_copy(din.at[pl.ds(1, NR - 1)], din.at[pl.ds(1, NR - 1)], d_sem.at[sem]).wait()

    @pl.loop(1, NR)
    def _(k):
        dsend(k).start()

    for source, by_y, by_z in ((s1h, s2h, rh), (s1l, s2l, rl)):
        @pl.loop(0, 16)
        def _(b):
            block = source[pl.ds(pl.multiple_of(b * 64, 64), 64), :]
            by_y[pl.ds(pl.multiple_of((b % 4) * 256 + (b // 4) * 64, 64), 64), :] = block
            wide_block = block.astype(F32)
            for z in range(4):
                pair = jnp.concatenate(
                    [wide_block[8 * z:8 * z + 8, :], wide_block[32 + 8 * z:40 + 8 * z, :]], axis=0)
                by_z[pl.ds(pl.multiple_of(z * 256 + b * 16, 16), 16), :] = pair.astype(BF16)

    with jax.named_scope("drecv"):
        others(1)

    total = dpart[r] + jnp.sum(din[pl.ds(1, NR - 1)], axis=0)
    din[0] = total
    dfull[r] = total

    @pl.loop(1, NR)
    def _(k):
        dback(k).start()

    def transposed(i):
        at = pl.multiple_of(i * 128, 128)
        strip = l1[pl.ds(i * 4, 4), :, :].reshape(128, N).T
        h, l = split(strip)
        l1th[:, pl.ds(at, 128)] = h
        l1tl[:, pl.ds(at, 128)] = l

    @pl.loop(0, N // 128)
    def _(i):
        transposed(i)

    with jax.named_scope("dback"):
        others(3)
    others(0)
    others(2)

    for t in range(8):
        cols = pl.ds(t * 128, 128)
        def body(p, acc):
            return acc + l1[p, :, cols] * dfull[p, pl.ds(t, 1), :]
        acc = lax.fori_loop(0, VECS, body, jnp.zeros((ROWS, 128), F32), unroll=4)
        own[:, :, cols] = acc.reshape(NV, 8, 128)

    full6 = full2.reshape(4, 4, 2, 4, 8, N)

    def own2(part, at, first):
        lo, n, order = PARTS[part]
        lanes = pl.ds(lo, n)
        rows = {
            "x": lambda: full6[at, :, :, :, :, lanes],
            "y": lambda: full6[:, at, :, :, :, lanes],
            "z": lambda: full6[:, :, :, at, :, lanes],
        }[order[2]]().reshape(256, n)
        sh, sl = {"x": (s1h, s1l), "y": (s2h, s2l), "z": (rh, rl)}[order[2]]
        h, l = split(rows.T)
        mh[pl.ds(0, n), :] = h
        ml[pl.ds(0, n), :] = l
        depth = pl.ds(pl.multiple_of(at * 256, 256), 256)

        @pl.loop(0, 2)
        def _(j):
            cols = pl.ds(pl.multiple_of(j * 512, 512), 512)
            res = dot3(mh[pl.ds(0, n), :], ml[pl.ds(0, n), :], sh[depth, cols], sl[depth, cols])
            if first:
                stage[lanes, cols] = res
            else:
                stage[lanes, cols] += res

    with jax.named_scope("ex2"):
        exchange(full2, 1, nothing, own2)

    with jax.named_scope("gen2"):
        scale2 = antisymmetric(stage, ah, al)

    def partner(i, way):
        dx, dy, dc = OFFSETS[i]
        return ((cx + way * dx + 4) % 4) * 8 + ((cy + way * dy + 4) % 4) * 2 + (cc + dc) % 2

    def rows_of(device):
        return pl.ds(pl.multiple_of(device * ROWS, ROWS), ROWS)

    def big(g, i):
        to = partner(i, 1)
        lanes = pl.ds(pl.multiple_of(g * GW, GW), GW)
        return pltpu.make_async_remote_copy(
            src_ref=stage.at[rows_of(to), lanes], dst_ref=zbuf.at[mine, lanes],
            send_sem=big_s, recv_sem=big_r.at[g, OFFSETS[i][0]],
            device_id=(v, to), device_id_type=MESH)

    def big_taken(g, dx):
        ref = zbuf.at[pl.ds(0, (8 if dx else 7) * ROWS), pl.ds(g * GW, GW)]
        pltpu.make_async_copy(ref, ref, big_r.at[g, dx]).wait()

    @pl.loop(0, GROUPS)
    def _(g):
        lanes = pl.ds(pl.multiple_of(g * GW, GW), GW)
        with jax.named_scope("l2"):
            h, l = split(scale2 * dot3(ah[...], al[...], l1th[:, lanes], l1tl[:, lanes]))
            wh[...] = h
            wl[...] = l
            stage[:, lanes] = dot3(ah[...], al[...], wh[...], wl[...])

            @pl.loop(0, 8)
            def _(i):
                rows = pl.ds(pl.multiple_of(i * 128, 128), 128)
                base = l1th[rows, lanes].astype(F32) + l1tl[rows, lanes].astype(F32)
                first = wh[rows, :].astype(F32) + wl[rows, :].astype(F32)
                stage[rows, lanes] = base + ((0.5 * scale2) * stage[rows, lanes] - first)
        for i in range(NR - 1):
            big(g, i).start()
        zbuf[mine, lanes] = stage[mine, lanes]

    def rotation(cols, j):
        h, l = split(dot3(s1h[...], s1l[...], s2h[:, cols], s2l[:, cols]))
        rh[:, cols] = h
        rl[:, cols] = l

    with jax.named_scope("step2"):
        series(scale2, s2h, s2l)
    with jax.named_scope("rot"):
        panels(rotation)
    rot_ref[...] = rh[mine, :].astype(F32) + rl[mine, :].astype(F32)

    group = lax.broadcasted_iota(jnp.int32, (ROWS, 128), 1) // ROWS

    def gathered(at, q, row, col):
        blocks = [
            zbuf[pl.ds(pl.multiple_of(at + b * ROWS, ROWS), ROWS), pl.ds(pl.multiple_of(q * 128, 128), 128)]
            for b in range(4)]
        for p in range(4):
            out = blocks[p]
            for b in range(4):
                if b != p:
                    turned = pltpu.roll(blocks[b], (ROWS * (b - p)) % 128, 1)
                    out = jnp.where(group == b, turned, out)
            h, l = split(out)
            rows = pl.ds(row + p * ROWS, ROWS)
            lh[rows, col] = h
            ll[rows, col] = l

    def finish(first, chunks):
        m = chunks * GW
        with jax.named_scope(f"bigwait{first}"):
            for g in range(first, first + chunks):
                for dx in range(4):
                    big_taken(g, dx)

        with jax.named_scope(f"turn{first}"):
            @pl.loop(0, 8)
            def _(b4):
                at = pl.multiple_of(b4 * 128, 128)
                for q in range(m // 128):
                    gathered(at, first * GW // 128 + q, q * 128, pl.ds(at, 128))

        with jax.named_scope(f"final{first}"):
            @pl.loop(0, 2)
            def _(j):
                cols = pl.ds(pl.multiple_of(j * 512, 512), 512)
                res = dot3(lh[pl.ds(0, m), :], ll[pl.ds(0, m), :], rh[:, cols], rl[:, cols])
                out_ref[pl.ds(first * GP, chunks * GP), :, cols] = res.reshape(chunks * GP, ROWS, 512)

    finish(0, 2)
    finish(2, 1)

    last = GROUPS - 1
    for dx in (1, 3, 0, 2):
        with jax.named_scope(f"bigwait3_{dx}"):
            big_taken(last, dx)
        at = pl.multiple_of(((cx + 4 - dx) % 4) * 256, 256)
        for b4 in range(2):
            for q in range(GW // 128):
                gathered(at + b4 * 128, last * GW // 128 + q, q * 128, pl.ds(b4 * 128, 128))

        @pl.loop(0, 2)
        def _(j):
            cols = pl.ds(pl.multiple_of(j * 512, 512), 512)
            depth, first = pl.ds(at, 256), pl.ds(0, GW)
            res = dot3(lh[first, pl.ds(0, 256)], ll[first, pl.ds(0, 256)], rh[depth, cols], rl[depth, cols])
            res = res.reshape(GP, ROWS, 512)
            if dx == 1:
                out_ref[pl.ds(last * GP, GP), :, cols] = res
            else:
                out_ref[pl.ds(last * GP, GP), :, cols] += res

    sent = stage.at[pl.ds(0, N - ROWS), :]
    pltpu.make_async_copy(sent, sent, big_s).wait()


def shards(chol_vectors):
    full = pltpu.VMEM((N, N), F32)
    half = pltpu.VMEM((N, N), BF16)
    sem = pltpu.SemaphoreType.DMA
    return pl.pallas_call(
        kernel,
        out_shape=(
            pltpu.VMEM((VECS, ROWS, N), F32),
            pltpu.VMEM((ROWS, N), F32),
        ),
        in_specs=[pl.BlockSpec(memory_space=pl.ANY)],
        out_specs=(pl.BlockSpec(memory_space=pltpu.VMEM), pl.BlockSpec(memory_space=pltpu.VMEM)),
        scratch_shapes=[
            pltpu.VMEM((VECS, ROWS, N), F32),
            pltpu.VMEM((VECS, ROWS, 128), F32),
            pltpu.VMEM((NV, 8, N), F32),
            pltpu.VMEM((2, NV - 1, 8, N), F32),
            full,
            full,
            full,
            half, half, half, half,
            pltpu.VMEM((VECS, ROWS, N), F32),
            half, half,
            pltpu.VMEM((VECS, 8, 128), F32),
            pltpu.VMEM((NR, 8, 128), F32),
            pltpu.VMEM((NR, 8, 128), F32),
            full,
            half, half,
            full,
            half, half,
            pltpu.VMEM((N, GW), BF16), pltpu.VMEM((N, GW), BF16),
            pltpu.VMEM((2 * GW, N), BF16), pltpu.VMEM((2 * GW, N), BF16),
            pltpu.VMEM((384, 256), BF16), pltpu.VMEM((384, 256), BF16),
            sem,
            sem((2,)), sem((2,)),
            sem((2,)), sem((2, 3, 5)),
            sem((2,)), sem((2, 3, 4)),
            sem((4,)),
            sem, sem((GROUPS, 4)),
        ],
        compiler_params=pltpu.CompilerParams(
            collective_id=0, has_side_effects=True, vmem_limit_bytes=VMEM_LIMIT
        ),
    )(chol_vectors)


def solution(mesh):
    return jax.shard_map(
        shards,
        mesh=mesh,
        in_specs=(P("vec", "row", None),),
        out_specs=(P("vec", "row", None), P("row", None)),
        check_vma=False,
    )
```

```python
import functools

import jax
import jax.numpy as jnp
from jax import lax
from jax.experimental import pallas as pl
from jax.experimental.pallas import tpu as pltpu
from jax.sharding import PartitionSpec as P

N = 1024
NV = 4
NR = 32
VECS = 32
ROWS = 32
GW = 256
CW = 128
CHUNKS = N // CW
STEP_GAIN = 0.2
VMEM_LIMIT = 58 << 20
PARTS = ((0, 384, "zyx"), (384, 384, "xzy"), (768, 256, "yxz"))
OFFSETS = tuple(sorted(
    ((dx, dy, dc) for dx in range(4) for dy in range(4) for dc in range(2) if dx or dy or dc),
    key=lambda o: -(min(o[0], 4 - o[0]) + min(o[1], 4 - o[1]))))
MESH = pl.DeviceIdType.MESH
F32 = jnp.float32
BF16 = jnp.bfloat16


def split(x):
    high = x.astype(BF16)
    return high, (x - high.astype(F32)).astype(BF16)


def dot3(ah, al, bh, bl):
    dot = functools.partial(jnp.dot, preferred_element_type=F32)
    return dot(ah, bh) + dot(ah, bl) + dot(al, bh)


def kernel(
    x_ref, out_ref, rot_ref,
    xf, dbuf, own, zin, full1, full2, gf, s1h, s1l, s2h, s2l,
    l1, l1th, l1tl, dpart, din, dfull, zbuf, ah, al, stage, rh, rl, wh, wl, lh, ll, mh, ml,
    x_sem, zs_s, zs_r, ag_s, ag_r, co_s, co_r, d_sem, big_s, big_r,
):
    v = lax.axis_index("vec")
    r = lax.axis_index("row")
    cx, cy, cc = r // 8, (r // 2) % 4, r % 2

    load = pltpu.make_async_copy(x_ref, xf, x_sem)
    load.start()
    barrier = pltpu.get_barrier_semaphore()

    @pl.loop(1, NR)
    def _(k):
        pl.semaphore_signal(barrier, inc=1, device_id=(v, (r + k) % NR), device_id_type=MESH)

    @pl.loop(1, NV)
    def _(k):
        pl.semaphore_signal(barrier, inc=1, device_id=((v + k) % NV, r), device_id_type=MESH)

    load.wait()

    window = pl.multiple_of((r // 4) * 128, 128)
    lane = lax.broadcasted_iota(jnp.int32, (8, ROWS, 128), 2)
    sub = lax.broadcasted_iota(jnp.int32, (8, ROWS, 128), 1)

    @pl.loop(0, VECS // 8)
    def _(g):
        block = xf[pl.ds(g * 8, 8), :, pl.ds(window, 128)]
        picked = jnp.where(lane == sub + (r % 4) * ROWS, block, 0.0)
        dbuf[pl.ds(g * 8, 8)] = jnp.broadcast_to(
            jnp.sum(picked, axis=2, keepdims=True), (8, ROWS, 128)
        )

    def weighted(source, weight_of):
        for t in range(0, N, 256):
            def body(p, acc):
                return acc + source(p, t) * weight_of(p, t)
            acc = lax.fori_loop(0, VECS, body, jnp.zeros((ROWS, 256), F32), unroll=4)
            own[:, :, pl.ds(t, 256)] = acc.reshape(NV, 8, 256)

    def wide(d):
        return jnp.concatenate([d, d], axis=1)

    weighted(lambda p, t: xf[p, :, pl.ds(t, 256)], lambda p, t: wide(dbuf[p]))
    pl.semaphore_wait(barrier, NR - 1 + NV - 1)

    def exchange(full, which, filler, consume=None):
        full6 = full.reshape(4, 4, 2, 4, 8, N)

        def zcopy(k):
            to = (v + k) % NV
            return pltpu.make_async_remote_copy(
                src_ref=own.at[to], dst_ref=zin.at[which, k - 1],
                send_sem=zs_s.at[which], recv_sem=zs_r.at[which],
                device_id=(to, r), device_id_type=MESH)

        zcopies = [zcopy(k) for k in range(1, NV)]
        for c in zcopies:
            c.start()
        def taken(ref, sem):
            pltpu.make_async_copy(ref, ref, sem).wait()

        taken(zin.at[which], zs_r.at[which])
        piece = own[v] + zin[which, 0] + zin[which, 1] + zin[which, 2]
        full6[cx, cy, cc, v] = piece

        def region(part, have, at):
            lo, n, _ = PARTS[part]
            ix, iy, iz = (
                pl.ds(0, 4) if d in have else pl.ds(at[d], 1) for d in "xyz")
            return full6.at[ix, iy, pl.ds(at["c"], 1), iz, :, pl.ds(lo, n)]

        me = dict(x=cx, y=cy, z=v, c=cc)

        def peer(d, k):
            at = dict(me)
            at[d] = (me[d] + k) % 4
            return at

        def device(at):
            return (at["z"], at["x"] * 8 + at["y"] * 2 + at["c"])

        def ag(part, phase, k):
            order = PARTS[part][2]
            have = order[:phase]
            return pltpu.make_async_remote_copy(
                src_ref=region(part, have, me), dst_ref=region(part, have, me),
                send_sem=ag_s.at[which], recv_sem=ag_r.at[which, part, phase + (k - 1 if phase == 2 else 0)],
                device_id=device(peer(order[phase], k)), device_id_type=MESH)

        def core(part, have, at, group):
            return pltpu.make_async_remote_copy(
                src_ref=region(part, have, at), dst_ref=region(part, have, at),
                send_sem=co_s.at[which], recv_sem=co_r.at[which, part, group],
                device_id=device(dict(me, c=1 - cc)), device_id_type=MESH)

        def lanes_taken(part, rows, sem):
            lo, n, _ = PARTS[part]
            taken(full.at[pl.ds(0, rows), pl.ds(lo, n)], sem)

        for phase in range(3):
            for part in range(3):
                order = PARTS[part][2]
                if phase:
                    lanes_taken(part, 24 * 4 ** (phase - 1), ag_r.at[which, part, phase - 1])
                    for k in (1, 3, 2):
                        core(part, order[:phase - 1], peer(order[phase - 1], k), 0).start()
                for k in ((1, 3, 2) if phase == 2 else (2, 1, 3)):
                    ag(part, phase, k).start()
                if phase == 0:
                    core(part, "", me, 0).start()
            filler(phase)

        def arrived(k):
            for part in range(3):
                order = PARTS[part][2]
                lanes_taken(part, 128, ag_r.at[which, part, 2 + k - 1])
                core(part, order[:2], peer(order[2], 4 - k), k).start()

        def use(k):
            for part in range(3):
                lanes_taken(part, 128, co_r.at[which, part, k])
                if consume is not None:
                    consume(part, peer(PARTS[part][2][2], (4 - k) % 4)[PARTS[part][2][2]], k == 0)

        with jax.named_scope(f"use{which}_0"):
            use(0)
        with jax.named_scope(f"arr{which}_13"):
            arrived(1)
            arrived(3)
        with jax.named_scope(f"use{which}_1"):
            use(1)
        with jax.named_scope(f"arr{which}_2"):
            arrived(2)
        with jax.named_scope(f"use{which}_3"):
            use(3)
        with jax.named_scope(f"use{which}_2"):
            use(2)
        taken(full.at[pl.ds(0, N // 2), :], co_s.at[which])
        taken(zin.at[which], zs_s.at[which])
        taken(full.at[pl.ds(0, N // 2 - 8), :], ag_s.at[which])

    def nothing(phase):
        pass

    xh, xl = l1th, l1tl

    def prepare(phase):
        if phase == 0:
            @pl.loop(0, VECS // 4)
            def _(i):
                h, l = split(xf[pl.ds(i * 4, 4)].reshape(128, N))
                rows = pl.ds(pl.multiple_of(i * 128, 128), 128)
                xh[rows, :] = h
                xl[rows, :] = l

    with jax.named_scope("ex1"):
        exchange(full1, 0, prepare)

    def antisymmetric(full, high, low):
        def body(i, acc):
            at = pl.multiple_of(i * 128, 128)
            strip = full[pl.ds(at, 128), :] - full[:, pl.ds(at, 128)].T
            gf[pl.ds(at, 128), :] = strip
            h, l = split(strip)
            high[pl.ds(at, 128), :] = h
            low[pl.ds(at, 128), :] = l
            square = strip * strip
            return acc + jnp.sum(square.reshape(16, 8, N), axis=0)
        acc = lax.fori_loop(0, N // 128, body, jnp.zeros((8, N), F32), unroll=2)
        total = jnp.sum(jnp.sum(acc, axis=1, keepdims=True), axis=0, keepdims=True)
        norm = jnp.sqrt(total / (N * N) + 1e-06)
        return (STEP_GAIN / (N ** 0.5)) / norm

    def eye(i, j, m, n):
        rows = lax.broadcasted_iota(jnp.int32, (m, n), 0) + i
        cols = lax.broadcasted_iota(jnp.int32, (m, n), 1) + j
        return (rows == cols).astype(F32)

    with jax.named_scope("gen1"):
        scale = antisymmetric(full1, ah, al)

    def panels(body):
        @pl.loop(0, N // 256)
        def _(t):
            body(pl.ds(pl.multiple_of(t * 256, 256), 256), t * 256)

    def series(c, high, low):
        def store(rows, cols, i, j, sq):
            value = c * gf[rows, cols] + (0.5 * c * c) * sq
            h, l = split(value + eye(i, j, sq.shape[0], 256) if i <= j else value)
            high[rows, cols] = h
            low[rows, cols] = l

        for t in range(4):
            m, cols = 256 * (t + 1), pl.ds(256 * t, 256)
            sq = dot3(ah[pl.ds(0, m), :], al[pl.ds(0, m), :], ah[:, cols], al[:, cols])
            store(pl.ds(0, m), cols, 0, 256 * t, sq)
            for u in range(t):
                store(cols, pl.ds(256 * u, 256), 256 * t, 256 * u, sq[256 * u:256 * (u + 1), :].T)

    with jax.named_scope("step1"):
        series(scale, s1h, s1l)

    def left(cols, j):
        l1[:, :, cols] = dot3(xh[...], xl[...], s1h[:, cols], s1l[:, cols]).reshape(VECS, ROWS, 256)

    with jax.named_scope("left"):
        panels(left)

    mine = pl.ds(pl.multiple_of(r * ROWS, ROWS), ROWS)
    for t in range(8):
        cols = pl.ds(t * 128, 128)
        weight = s1h[mine, cols].astype(F32) + s1l[mine, cols].astype(F32)

        @pl.loop(0, VECS, unroll=16)
        def _(p):
            dpart[p, pl.ds(t, 1), :] = jnp.sum(l1[p, :, cols] * weight, axis=0, keepdims=True)

    def dsend(k):
        to = (r + k) % NR
        return pltpu.make_async_remote_copy(
            src_ref=dpart.at[to], dst_ref=din.at[k], send_sem=d_sem.at[0], recv_sem=d_sem.at[1],
            device_id=(v, to), device_id_type=MESH)

    def dback(k):
        to = (r + k) % NR
        return pltpu.make_async_remote_copy(
            src_ref=din.at[0], dst_ref=dfull.at[r], send_sem=d_sem.at[2], recv_sem=d_sem.at[3],
            device_id=(v, to), device_id_type=MESH)

    def others(sem):
        pltpu.make_async_copy(din.at[pl.ds(1, NR - 1)], din.at[pl.ds(1, NR - 1)], d_sem.at[sem]).wait()

    @pl.loop(1, NR)
    def _(k):
        dsend(k).start()

    for source, by_y, by_z in ((s1h, s2h, rh), (s1l, s2l, rl)):
        @pl.loop(0, 16)
        def _(b):
            block = source[pl.ds(pl.multiple_of(b * 64, 64), 64), :]
            by_y[pl.ds(pl.multiple_of((b % 4) * 256 + (b // 4) * 64, 64), 64), :] = block
            wide_block = block.astype(F32)
            for z in range(4):
                pair = jnp.concatenate(
                    [wide_block[8 * z:8 * z + 8, :], wide_block[32 + 8 * z:40 + 8 * z, :]], axis=0)
                by_z[pl.ds(pl.multiple_of(z * 256 + b * 16, 16), 16), :] = pair.astype(BF16)

    with jax.named_scope("drecv"):
        others(1)

    total = dpart[r] + jnp.sum(din[pl.ds(1, NR - 1)], axis=0)
    din[0] = total
    dfull[r] = total

    @pl.loop(1, NR)
    def _(k):
        dback(k).start()

    def transposed(i):
        at = pl.multiple_of(i * 128, 128)
        strip = l1[pl.ds(i * 4, 4), :, :].reshape(128, N).T
        h, l = split(strip)
        l1th[:, pl.ds(at, 128)] = h
        l1tl[:, pl.ds(at, 128)] = l

    @pl.loop(0, N // 128)
    def _(i):
        transposed(i)

    with jax.named_scope("dback"):
        others(3)
    others(0)
    others(2)

    for t in range(8):
        cols = pl.ds(t * 128, 128)
        def body(p, acc):
            return acc + l1[p, :, cols] * dfull[p, pl.ds(t, 1), :]
        acc = lax.fori_loop(0, VECS, body, jnp.zeros((ROWS, 128), F32), unroll=4)
        own[:, :, cols] = acc.reshape(NV, 8, 128)

    full6 = full2.reshape(4, 4, 2, 4, 8, N)

    def own2(part, at, first):
        lo, n, order = PARTS[part]
        lanes = pl.ds(lo, n)
        rows = {
            "x": lambda: full6[at, :, :, :, :, lanes],
            "y": lambda: full6[:, at, :, :, :, lanes],
            "z": lambda: full6[:, :, :, at, :, lanes],
        }[order[2]]().reshape(256, n)
        sh, sl = {"x": (s1h, s1l), "y": (s2h, s2l), "z": (rh, rl)}[order[2]]
        h, l = split(rows.T)
        mh[pl.ds(0, n), :] = h
        ml[pl.ds(0, n), :] = l
        depth = pl.ds(pl.multiple_of(at * 256, 256), 256)

        res = dot3(mh[pl.ds(0, n), :], ml[pl.ds(0, n), :], sh[depth, :], sl[depth, :])
        if first:
            stage[lanes, :] = res
        else:
            stage[lanes, :] += res

    with jax.named_scope("ex2"):
        exchange(full2, 1, nothing, own2)

    with jax.named_scope("gen2"):
        scale2 = antisymmetric(stage, ah, al)

    def partner(i, way):
        dx, dy, dc = OFFSETS[i]
        return ((cx + way * dx + 4) % 4) * 8 + ((cy + way * dy + 4) % 4) * 2 + (cc + dc) % 2

    def rows_of(device):
        return pl.ds(pl.multiple_of(device * ROWS, ROWS), ROWS)

    def big(g, i):
        to = partner(i, 1)
        lanes = pl.ds(pl.multiple_of(g * CW, CW), CW)
        return pltpu.make_async_remote_copy(
            src_ref=stage.at[rows_of(to), lanes], dst_ref=zbuf.at[mine, lanes],
            send_sem=big_s, recv_sem=big_r.at[g],
            device_id=(v, to), device_id_type=MESH)

    @pl.loop(0, N // GW)
    def _(g):
        lanes = pl.ds(pl.multiple_of(g * GW, GW), GW)
        with jax.named_scope("l2"):
            for u in range(2):
                rows = pl.ds(u * 512, 512)
                h, l = split(scale2 * dot3(ah[rows, :], al[rows, :], l1th[:, lanes], l1tl[:, lanes]))
                wh[rows, :] = h
                wl[rows, :] = l
            for u in range(2):
                rows = pl.ds(u * 512, 512)
                stage[rows, lanes] = dot3(ah[rows, :], al[rows, :], wh[...], wl[...])

            @pl.loop(0, 8)
            def _(i):
                rows = pl.ds(pl.multiple_of(i * 128, 128), 128)
                base = l1th[rows, lanes].astype(F32) + l1tl[rows, lanes].astype(F32)
                first = wh[rows, :].astype(F32) + wl[rows, :].astype(F32)
                stage[rows, lanes] = base + ((0.5 * scale2) * stage[rows, lanes] - first)

        for u in range(GW // CW):
            for i in range(NR - 1):
                big(g * (GW // CW) + u, i).start()
        zbuf[mine, lanes] = stage[mine, lanes]

    def rotation(cols, j):
        h, l = split(dot3(s1h[...], s1l[...], s2h[:, cols], s2l[:, cols]))
        rh[:, cols] = h
        rl[:, cols] = l

    with jax.named_scope("step2"):
        series(scale2, s2h, s2l)
    with jax.named_scope("rot"):
        panels(rotation)
    rot_ref[...] = rh[mine, :].astype(F32) + rl[mine, :].astype(F32)

    group = lax.broadcasted_iota(jnp.int32, (ROWS, 128), 1) // ROWS

    def gathered(at, q, row, col):
        blocks = [
            zbuf[pl.ds(pl.multiple_of(at + b * ROWS, ROWS), ROWS), pl.ds(pl.multiple_of(q * 128, 128), 128)]
            for b in range(4)]
        for p in range(4):
            out = blocks[p]
            for b in range(4):
                if b != p:
                    turned = pltpu.roll(blocks[b], (ROWS * (b - p)) % 128, 1)
                    out = jnp.where(group == b, turned, out)
            h, l = split(out)
            rows = pl.ds(row + p * ROWS, ROWS)
            lh[rows, col] = h
            ll[rows, col] = l

    def finish(first, chunks, width):
        m = chunks * CW
        with jax.named_scope(f"bigwait{first}"):
            for g in range(first, first + chunks):
                ref = zbuf.at[pl.ds(0, N - ROWS), pl.ds(g * CW, CW)]
                pltpu.make_async_copy(ref, ref, big_r.at[g]).wait()

        with jax.named_scope(f"turn{first}"):
            @pl.loop(0, 8, unroll=2 if chunks == 1 else None)
            def _(b4):
                at = pl.multiple_of(b4 * 128, 128)
                for q in range(chunks):
                    gathered(at, first + q, q * 128, pl.ds(at, 128))

        with jax.named_scope(f"final{first}"):
            @pl.loop(0, N // width)
            def _(j):
                cols = pl.ds(pl.multiple_of(j * width, width), width)
                res = dot3(lh[pl.ds(0, m), :], ll[pl.ds(0, m), :], rh[:, cols], rl[:, cols])
                out_ref[pl.ds(first * 4, chunks * 4), :, cols] = res.reshape(chunks * 4, ROWS, width)

    finish(0, 4, 512)
    finish(4, 2, 512)
    finish(6, 1, 1024)
    finish(7, 1, 1024)

    sent = stage.at[pl.ds(0, N - ROWS), :]
    pltpu.make_async_copy(sent, sent, big_s).wait()


def shards(chol_vectors):
    full = pltpu.VMEM((N, N), F32)
    half = pltpu.VMEM((N, N), BF16)
    sem = pltpu.SemaphoreType.DMA
    return pl.pallas_call(
        kernel,
        out_shape=(
            pltpu.VMEM((VECS, ROWS, N), F32),
            pltpu.VMEM((ROWS, N), F32),
        ),
        in_specs=[pl.BlockSpec(memory_space=pl.ANY)],
        out_specs=(pl.BlockSpec(memory_space=pltpu.VMEM), pl.BlockSpec(memory_space=pltpu.VMEM)),
        scratch_shapes=[
            pltpu.VMEM((VECS, ROWS, N), F32),
            pltpu.VMEM((VECS, ROWS, 128), F32),
            pltpu.VMEM((NV, 8, N), F32),
            pltpu.VMEM((2, NV - 1, 8, N), F32),
            full,
            full,
            full,
            half, half, half, half,
            pltpu.VMEM((VECS, ROWS, N), F32),
            half, half,
            pltpu.VMEM((VECS, 8, 128), F32),
            pltpu.VMEM((NR, 8, 128), F32),
            pltpu.VMEM((NR, 8, 128), F32),
            full,
            half, half,
            full,
            half, half,
            pltpu.VMEM((N, GW), BF16), pltpu.VMEM((N, GW), BF16),
            pltpu.VMEM((2 * GW, N), BF16), pltpu.VMEM((2 * GW, N), BF16),
            pltpu.VMEM((384, 256), BF16), pltpu.VMEM((384, 256), BF16),
            sem,
            sem((2,)), sem((2,)),
            sem((2,)), sem((2, 3, 5)),
            sem((2,)), sem((2, 3, 4)),
            sem((4,)),
            sem, sem((CHUNKS,)),
        ],
        compiler_params=pltpu.CompilerParams(
            collective_id=0, has_side_effects=True, vmem_limit_bytes=VMEM_LIMIT
        ),
    )(chol_vectors)


def solution(mesh):
    return jax.shard_map(
        shards,
        mesh=mesh,
        in_specs=(P("vec", "row", None),),
        out_specs=(P("vec", "row", None), P("row", None)),
        check_vma=False,
    )
```

```python
import functools

import jax
import jax.numpy as jnp
from jax import lax
from jax.experimental import pallas as pl
from jax.experimental.pallas import tpu as pltpu
from jax.sharding import PartitionSpec as P

N = 1024
NV = 4
NR = 32
VECS = 32
ROWS = 32
GW = 256
CW = 128
CHUNKS = N // CW
STEP_GAIN = 0.2
VMEM_LIMIT = 54 << 20
PARTS = ((0, 384, "zyx"), (384, 384, "xzy"), (768, 256, "yxz"))
OFFSETS = tuple(sorted(
    ((dx, dy, dc) for dx in range(4) for dy in range(4) for dc in range(2) if dx or dy or dc),
    key=lambda o: -(min(o[0], 4 - o[0]) + min(o[1], 4 - o[1]))))
MESH = pl.DeviceIdType.MESH
F32 = jnp.float32
BF16 = jnp.bfloat16


def split(x):
    high = x.astype(BF16)
    return high, (x - high.astype(F32)).astype(BF16)


def dot3(ah, al, bh, bl):
    dot = functools.partial(jnp.dot, preferred_element_type=F32)
    return dot(ah, bh) + dot(ah, bl) + dot(al, bh)


def gathered(z, high, low, at, lane, row):
    group = lax.broadcasted_iota(jnp.int32, (ROWS, 128), 1) // ROWS
    blocks = [
        z[pl.ds(pl.multiple_of(at + b * ROWS, ROWS), ROWS), pl.ds(pl.multiple_of(lane, 128), 128)]
        for b in range(4)]
    for p in range(4):
        out = blocks[p]
        for b in range(4):
            if b != p:
                turned = pltpu.roll(blocks[b], (ROWS * (b - p)) % 128, 1)
                out = jnp.where(group == b, turned, out)
        h, l = split(out)
        rows = pl.ds(row + p * ROWS, ROWS)
        high[rows, pl.ds(at, 128)] = h
        low[rows, pl.ds(at, 128)] = l


def tail(done_ref, rot_in, last_ref, rh, rl, out_ref, rot_ref, lh, ll, res, sems):
    held = VECS - 4
    copies = [
        pltpu.make_async_copy(done_ref.at[pl.ds(g * 7, 7)], out_ref.at[pl.ds(g * 7, 7)], sems.at[g])
        for g in range(held // 7)]
    copies.append(pltpu.make_async_copy(rot_in, rot_ref, sems.at[4]))
    for copy in copies:
        copy.start()

    @pl.loop(0, 8, unroll=2)
    def _(b4):
        gathered(last_ref, lh, ll, pl.multiple_of(b4 * 128, 128), 0, 0)

    res[...] = dot3(lh[...], ll[...], rh[...], rl[...]).reshape(4, ROWS, N)
    copies.append(pltpu.make_async_copy(res, out_ref.at[pl.ds(held, 4)], sems.at[5]))
    copies[-1].start()
    for copy in copies:
        copy.wait()


def kernel(
    x_ref, out_ref, rot_ref, last_ref, rh, rl,
    xf, dbuf, own, zin, full1, full2, gf, s1h, s1l, s2h, s2l,
    l1, l1th, l1tl, dpart, din, dfull, zbuf, ah, al, stage, wh, wl, lh, ll, mh, ml,
    x_sem, zs_s, zs_r, ag_s, ag_r, co_s, co_r, d_sem, big_s, big_r,
):
    v = lax.axis_index("vec")
    r = lax.axis_index("row")
    cx, cy, cc = r // 8, (r // 2) % 4, r % 2

    loads = [
        pltpu.make_async_copy(x_ref.at[pl.ds(g * 8, 8)], xf.at[pl.ds(g * 8, 8)], x_sem.at[g])
        for g in range(VECS // 8)]
    for load in loads:
        load.start()

    def partner(i, way):
        dx, dy, dc = OFFSETS[i]
        return ((cx + way * dx + 4) % 4) * 8 + ((cy + way * dy + 4) % 4) * 2 + (cc + dc) % 2

    barrier = pltpu.get_barrier_semaphore()
    for i in range(NR - 1):
        pl.semaphore_signal(barrier, inc=1, device_id=(v, partner(i, 1)), device_id_type=MESH)
    for k in range(1, NV):
        pl.semaphore_signal(barrier, inc=1, device_id=((v + k) % NV, r), device_id_type=MESH)

    window = pl.multiple_of((r // 4) * 128, 128)
    lane = lax.broadcasted_iota(jnp.int32, (8, ROWS, 128), 2)
    sub = lax.broadcasted_iota(jnp.int32, (8, ROWS, 128), 1)

    for g, load in enumerate(loads):
        load.wait()
        block = xf[pl.ds(g * 8, 8), :, pl.ds(window, 128)]
        picked = jnp.where(lane == sub + (r % 4) * ROWS, block, 0.0)
        dbuf[pl.ds(g * 8, 8)] = jnp.broadcast_to(
            jnp.sum(picked, axis=2, keepdims=True), (8, ROWS, 128)
        )

    def weighted(source, weight_of):
        for t in range(0, N, 256):
            def body(p, acc):
                return acc + source(p, t) * weight_of(p, t)
            acc = lax.fori_loop(0, VECS, body, jnp.zeros((ROWS, 256), F32), unroll=4)
            own[:, :, pl.ds(t, 256)] = acc.reshape(NV, 8, 256)

    def wide(d):
        return jnp.concatenate([d, d], axis=1)

    weighted(lambda p, t: xf[p, :, pl.ds(t, 256)], lambda p, t: wide(dbuf[p]))
    pl.semaphore_wait(barrier, NR - 1 + NV - 1)

    def exchange(full, which, filler, consume=None):
        full6 = full.reshape(4, 4, 2, 4, 8, N)

        def zcopy(k):
            to = (v + k) % NV
            return pltpu.make_async_remote_copy(
                src_ref=own.at[to], dst_ref=zin.at[which, k - 1],
                send_sem=zs_s.at[which], recv_sem=zs_r.at[which],
                device_id=(to, r), device_id_type=MESH)

        zcopies = [zcopy(k) for k in range(1, NV)]
        for c in zcopies:
            c.start()
        def taken(ref, sem):
            pltpu.make_async_copy(ref, ref, sem).wait()

        taken(zin.at[which], zs_r.at[which])
        piece = own[v] + zin[which, 0] + zin[which, 1] + zin[which, 2]
        full6[cx, cy, cc, v] = piece

        def region(part, have, at):
            lo, n, _ = PARTS[part]
            ix, iy, iz = (
                pl.ds(0, 4) if d in have else pl.ds(at[d], 1) for d in "xyz")
            return full6.at[ix, iy, pl.ds(at["c"], 1), iz, :, pl.ds(lo, n)]

        me = dict(x=cx, y=cy, z=v, c=cc)

        def peer(d, k):
            at = dict(me)
            at[d] = (me[d] + k) % 4
            return at

        def device(at):
            return (at["z"], at["x"] * 8 + at["y"] * 2 + at["c"])

        def ag(part, phase, k):
            order = PARTS[part][2]
            have = order[:phase]
            return pltpu.make_async_remote_copy(
                src_ref=region(part, have, me), dst_ref=region(part, have, me),
                send_sem=ag_s.at[which], recv_sem=ag_r.at[which, part, phase + (k - 1 if phase == 2 else 0)],
                device_id=device(peer(order[phase], k)), device_id_type=MESH)

        def core(part, have, at, group):
            return pltpu.make_async_remote_copy(
                src_ref=region(part, have, at), dst_ref=region(part, have, at),
                send_sem=co_s.at[which], recv_sem=co_r.at[which, part, group],
                device_id=device(dict(me, c=1 - cc)), device_id_type=MESH)

        def lanes_taken(part, rows, sem):
            lo, n, _ = PARTS[part]
            taken(full.at[pl.ds(0, rows), pl.ds(lo, n)], sem)

        for phase in range(3):
            for part in range(3):
                order = PARTS[part][2]
                if phase:
                    lanes_taken(part, 24 * 4 ** (phase - 1), ag_r.at[which, part, phase - 1])
                    for k in (1, 3, 2):
                        core(part, order[:phase - 1], peer(order[phase - 1], k), 0).start()
                for k in ((1, 3, 2) if phase == 2 else (2, 1, 3)):
                    ag(part, phase, k).start()
                if phase == 0:
                    core(part, "", me, 0).start()
            filler(phase)

        def arrived(k):
            for part in range(3):
                order = PARTS[part][2]
                lanes_taken(part, 128, ag_r.at[which, part, 2 + k - 1])
                core(part, order[:2], peer(order[2], 4 - k), k).start()

        def use(k):
            for part in range(3):
                lanes_taken(part, 128, co_r.at[which, part, k])
                if consume is not None:
                    consume(part, peer(PARTS[part][2][2], (4 - k) % 4)[PARTS[part][2][2]], k == 0)

        with jax.named_scope(f"use{which}_0"):
            use(0)
        with jax.named_scope(f"arr{which}_13"):
            arrived(1)
            arrived(3)
        with jax.named_scope(f"use{which}_1"):
            use(1)
        with jax.named_scope(f"arr{which}_2"):
            arrived(2)
        with jax.named_scope(f"use{which}_3"):
            use(3)
        with jax.named_scope(f"use{which}_2"):
            use(2)
        taken(full.at[pl.ds(0, N // 2), :], co_s.at[which])
        taken(zin.at[which], zs_s.at[which])
        taken(full.at[pl.ds(0, N // 2 - 8), :], ag_s.at[which])

    def nothing(phase):
        pass

    xh, xl = l1th, l1tl

    def prepare(phase):
        if phase == 0:
            @pl.loop(0, VECS // 4)
            def _(i):
                h, l = split(xf[pl.ds(i * 4, 4)].reshape(128, N))
                rows = pl.ds(pl.multiple_of(i * 128, 128), 128)
                xh[rows, :] = h
                xl[rows, :] = l

    with jax.named_scope("ex1"):
        exchange(full1, 0, prepare)

    def antisymmetric(full, high, low):
        def body(i, acc):
            at = pl.multiple_of(i * 128, 128)
            strip = full[pl.ds(at, 128), :] - full[:, pl.ds(at, 128)].T
            gf[pl.ds(at, 128), :] = strip
            h, l = split(strip)
            high[pl.ds(at, 128), :] = h
            low[pl.ds(at, 128), :] = l
            square = strip * strip
            return acc + jnp.sum(square.reshape(16, 8, N), axis=0)
        acc = lax.fori_loop(0, N // 128, body, jnp.zeros((8, N), F32), unroll=2)
        total = jnp.sum(jnp.sum(acc, axis=1, keepdims=True), axis=0, keepdims=True)
        norm = jnp.sqrt(total / (N * N) + 1e-06)
        return (STEP_GAIN / (N ** 0.5)) / norm

    def eye(i, j, m, n):
        rows = lax.broadcasted_iota(jnp.int32, (m, n), 0) + i
        cols = lax.broadcasted_iota(jnp.int32, (m, n), 1) + j
        return (rows == cols).astype(F32)

    with jax.named_scope("gen1"):
        scale = antisymmetric(full1, ah, al)

    def panels(body):
        @pl.loop(0, N // 256)
        def _(t):
            body(pl.ds(pl.multiple_of(t * 256, 256), 256), t * 256)

    def series(c, high, low):
        def store(rows, cols, i, j, sq):
            value = c * gf[rows, cols] + (0.5 * c * c) * sq
            h, l = split(value + eye(i, j, sq.shape[0], 256) if i <= j else value)
            high[rows, cols] = h
            low[rows, cols] = l

        for t in range(4):
            m, cols = 256 * (t + 1), pl.ds(256 * t, 256)
            sq = dot3(ah[pl.ds(0, m), :], al[pl.ds(0, m), :], ah[:, cols], al[:, cols])
            store(pl.ds(0, m), cols, 0, 256 * t, sq)
            for u in range(t):
                store(cols, pl.ds(256 * u, 256), 256 * t, 256 * u, sq[256 * u:256 * (u + 1), :].T)

    with jax.named_scope("step1"):
        series(scale, s1h, s1l)

    def left(cols, j):
        l1[:, :, cols] = dot3(xh[...], xl[...], s1h[:, cols], s1l[:, cols]).reshape(VECS, ROWS, 256)

    with jax.named_scope("left"):
        panels(left)

    mine = pl.ds(pl.multiple_of(r * ROWS, ROWS), ROWS)
    for t in range(8):
        cols = pl.ds(t * 128, 128)
        weight = s1h[mine, cols].astype(F32) + s1l[mine, cols].astype(F32)

        @pl.loop(0, VECS, unroll=16)
        def _(p):
            dpart[p, pl.ds(t, 1), :] = jnp.sum(l1[p, :, cols] * weight, axis=0, keepdims=True)

    def dsend(i):
        to = partner(i, 1)
        return pltpu.make_async_remote_copy(
            src_ref=dpart.at[to], dst_ref=din.at[i + 1], send_sem=d_sem.at[0], recv_sem=d_sem.at[1],
            device_id=(v, to), device_id_type=MESH)

    def dback(i):
        to = partner(i, 1)
        return pltpu.make_async_remote_copy(
            src_ref=din.at[0], dst_ref=dfull.at[r], send_sem=d_sem.at[2], recv_sem=d_sem.at[3],
            device_id=(v, to), device_id_type=MESH)

    def others(sem):
        pltpu.make_async_copy(din.at[pl.ds(1, NR - 1)], din.at[pl.ds(1, NR - 1)], d_sem.at[sem]).wait()

    for i in range(NR - 1):
        dsend(i).start()

    for source, by_y, by_z in ((s1h, s2h, rh), (s1l, s2l, rl)):
        @pl.loop(0, 16)
        def _(b):
            block = source[pl.ds(pl.multiple_of(b * 64, 64), 64), :]
            by_y[pl.ds(pl.multiple_of((b % 4) * 256 + (b // 4) * 64, 64), 64), :] = block
            wide_block = block.astype(F32)
            for z in range(4):
                pair = jnp.concatenate(
                    [wide_block[8 * z:8 * z + 8, :], wide_block[32 + 8 * z:40 + 8 * z, :]], axis=0)
                by_z[pl.ds(pl.multiple_of(z * 256 + b * 16, 16), 16), :] = pair.astype(BF16)

    with jax.named_scope("drecv"):
        others(1)

    total = dpart[r] + jnp.sum(din[pl.ds(1, NR - 1)], axis=0)
    din[0] = total
    dfull[r] = total

    for i in range(NR - 1):
        dback(i).start()

    def transposed(i):
        at = pl.multiple_of(i * 128, 128)
        strip = l1[pl.ds(i * 4, 4), :, :].reshape(128, N).T
        h, l = split(strip)
        l1th[:, pl.ds(at, 128)] = h
        l1tl[:, pl.ds(at, 128)] = l

    @pl.loop(0, N // 128)
    def _(i):
        transposed(i)

    with jax.named_scope("dback"):
        others(3)
    others(0)
    others(2)

    for t in range(8):
        cols = pl.ds(t * 128, 128)
        def body(p, acc):
            return acc + l1[p, :, cols] * dfull[p, pl.ds(t, 1), :]
        acc = lax.fori_loop(0, VECS, body, jnp.zeros((ROWS, 128), F32), unroll=4)
        own[:, :, cols] = acc.reshape(NV, 8, 128)

    full6 = full2.reshape(4, 4, 2, 4, 8, N)

    def own2(part, at, first):
        lo, n, order = PARTS[part]
        lanes = pl.ds(lo, n)
        rows = {
            "x": lambda: full6[at, :, :, :, :, lanes],
            "y": lambda: full6[:, at, :, :, :, lanes],
            "z": lambda: full6[:, :, :, at, :, lanes],
        }[order[2]]().reshape(256, n)
        sh, sl = {"x": (s1h, s1l), "y": (s2h, s2l), "z": (rh, rl)}[order[2]]
        h, l = split(rows.T)
        mh[pl.ds(0, n), :] = h
        ml[pl.ds(0, n), :] = l
        depth = pl.ds(pl.multiple_of(at * 256, 256), 256)

        res = dot3(mh[pl.ds(0, n), :], ml[pl.ds(0, n), :], sh[depth, :], sl[depth, :])
        if first:
            stage[lanes, :] = res
        else:
            stage[lanes, :] += res

    with jax.named_scope("ex2"):
        exchange(full2, 1, nothing, own2)

    with jax.named_scope("gen2"):
        scale2 = antisymmetric(stage, ah, al)

    def rows_of(device):
        return pl.ds(pl.multiple_of(device * ROWS, ROWS), ROWS)

    def big(g, i):
        to = partner(i, 1)
        lanes = pl.ds(pl.multiple_of(g * CW, CW), CW)
        return pltpu.make_async_remote_copy(
            src_ref=stage.at[rows_of(to), lanes], dst_ref=zbuf.at[mine, lanes],
            send_sem=big_s, recv_sem=big_r.at[g],
            device_id=(v, to), device_id_type=MESH)

    @pl.loop(0, N // GW)
    def _(g):
        lanes = pl.ds(pl.multiple_of(g * GW, GW), GW)
        with jax.named_scope("l2"):
            for u in range(2):
                rows = pl.ds(u * 512, 512)
                h, l = split(scale2 * dot3(ah[rows, :], al[rows, :], l1th[:, lanes], l1tl[:, lanes]))
                wh[rows, :] = h
                wl[rows, :] = l
            for u in range(2):
                rows = pl.ds(u * 512, 512)
                stage[rows, lanes] = dot3(ah[rows, :], al[rows, :], wh[...], wl[...])

            @pl.loop(0, 8)
            def _(i):
                rows = pl.ds(pl.multiple_of(i * 128, 128), 128)
                base = l1th[rows, lanes].astype(F32) + l1tl[rows, lanes].astype(F32)
                first = wh[rows, :].astype(F32) + wl[rows, :].astype(F32)
                stage[rows, lanes] = base + ((0.5 * scale2) * stage[rows, lanes] - first)

        for u in range(GW // CW):
            for i in range(NR - 1):
                big(g * (GW // CW) + u, i).start()
        zbuf[mine, lanes] = stage[mine, lanes]

    def rotation(cols, j):
        h, l = split(dot3(s1h[...], s1l[...], s2h[:, cols], s2l[:, cols]))
        rh[:, cols] = h
        rl[:, cols] = l

    with jax.named_scope("step2"):
        series(scale2, s2h, s2l)
    with jax.named_scope("rot"):
        panels(rotation)
    rot_ref[...] = rh[mine, :].astype(F32) + rl[mine, :].astype(F32)

    def finish(first, chunks, width):
        m = chunks * CW
        with jax.named_scope(f"bigwait{first}"):
            for g in range(first, first + chunks):
                ref = zbuf.at[pl.ds(0, N - ROWS), pl.ds(g * CW, CW)]
                pltpu.make_async_copy(ref, ref, big_r.at[g]).wait()

        with jax.named_scope(f"turn{first}"):
            @pl.loop(0, 8, unroll=2 if chunks == 1 else None)
            def _(b4):
                at = pl.multiple_of(b4 * 128, 128)
                for q in range(chunks):
                    gathered(zbuf, lh, ll, at, (first + q) * 128, q * 128)

        with jax.named_scope(f"final{first}"):
            @pl.loop(0, N // width)
            def _(j):
                cols = pl.ds(pl.multiple_of(j * width, width), width)
                res = dot3(lh[pl.ds(0, m), :], ll[pl.ds(0, m), :], rh[:, cols], rl[:, cols])
                out_ref[pl.ds(first * 4, chunks * 4), :, cols] = res.reshape(chunks * 4, ROWS, width)

    finish(0, 4, 512)
    finish(4, 2, 512)
    finish(6, 1, 1024)
    ref = zbuf.at[pl.ds(0, N - ROWS), pl.ds(0, CW)]
    pltpu.make_async_copy(ref, ref, big_r.at[CHUNKS - 1]).wait()
    last_ref[...] = zbuf[:, pl.ds(N - CW, CW)]

    sent = stage.at[pl.ds(0, N - ROWS), :]
    pltpu.make_async_copy(sent, sent, big_s).wait()


def shards(chol_vectors):
    full = pltpu.VMEM((N, N), F32)
    half = pltpu.VMEM((N, N), BF16)
    sem = pltpu.SemaphoreType.DMA
    outs = pl.pallas_call(
        kernel,
        out_shape=(
            pltpu.VMEM((VECS, ROWS, N), F32),
            pltpu.VMEM((ROWS, N), F32),
            pltpu.VMEM((N, CW), F32), half, half,
        ),
        in_specs=[pl.BlockSpec(memory_space=pl.ANY)],
        out_specs=(pl.BlockSpec(memory_space=pltpu.VMEM),) * 5,
        scratch_shapes=[
            pltpu.VMEM((VECS, ROWS, N), F32),
            pltpu.VMEM((VECS, ROWS, 128), F32),
            pltpu.VMEM((NV, 8, N), F32),
            pltpu.VMEM((2, NV - 1, 8, N), F32),
            full,
            full,
            full,
            half, half, half, half,
            pltpu.VMEM((VECS, ROWS, N), F32),
            half, half,
            pltpu.VMEM((VECS, 8, 128), F32),
            pltpu.VMEM((NR, 8, 128), F32),
            pltpu.VMEM((NR, 8, 128), F32),
            full,
            half, half,
            full,
            pltpu.VMEM((N, GW), BF16), pltpu.VMEM((N, GW), BF16),
            pltpu.VMEM((2 * GW, N), BF16), pltpu.VMEM((2 * GW, N), BF16),
            pltpu.VMEM((384, 256), BF16), pltpu.VMEM((384, 256), BF16),
            sem((VECS // 8,)),
            sem((2,)), sem((2,)),
            sem((2,)), sem((2, 3, 5)),
            sem((2,)), sem((2, 3, 4)),
            sem((4,)),
            sem, sem((CHUNKS,)),
        ],
        compiler_params=pltpu.CompilerParams(
            collective_id=0, has_side_effects=True, vmem_limit_bytes=VMEM_LIMIT
        ),
    )(chol_vectors)
    return pl.pallas_call(
        tail,
        out_shape=(
            jax.ShapeDtypeStruct((VECS, ROWS, N), F32),
            jax.ShapeDtypeStruct((ROWS, N), F32),
        ),
        in_specs=[pl.BlockSpec(memory_space=pltpu.VMEM)] * 5,
        out_specs=(pl.BlockSpec(memory_space=pl.ANY), pl.BlockSpec(memory_space=pl.ANY)),
        scratch_shapes=[
            pltpu.VMEM((CW, N), BF16), pltpu.VMEM((CW, N), BF16),
            pltpu.VMEM((4, ROWS, N), F32), sem((6,)),
        ],
        compiler_params=pltpu.CompilerParams(vmem_limit_bytes=8 << 20),
    )(*outs)


def solution(mesh):
    return jax.shard_map(
        shards,
        mesh=mesh,
        in_specs=(P("vec", "row", None),),
        out_specs=(P("vec", "row", None), P("row", None)),
        check_vma=False,
    )
```
